16 devices in a mesh: dp: 4 (over z, y), tp: 4 (over x, core).
Axes of the slice: x: 2, y: 2, z: 2, core: 2. Of those that a mesh axis runs over, the one named last changes fastest.
Arguments:
- x_in: bfloat16 [4096, 3584], P('dp'), parts along dimension 0
- lengths: int32 [4096], P('dp'), parts along dimension 0
- norm_gain: bfloat16 [2, 3584], replicated
- w_q: bfloat16 [2, 3584, 3584], P(None, None, 'tp')
- w_k: bfloat16 [2, 3584, 512], P(None, None, 'tp')
- w_v: bfloat16 [2, 3584, 512], P(None, None, 'tp')
- w_o: bfloat16 [2, 3584, 3584], P(None, 'tp')
- w_gate: bfloat16 [2, 3584, 18944], P(None, None, 'tp')
- w_up: bfloat16 [2, 3584, 18944], P(None, None, 'tp')
- w_down: bfloat16 [2, 18944, 3584], P(None, 'tp')
- k_cache: bfloat16 [2, 4096, 32, 4, 128], P(None, 'dp', None, 'tp'), parts along dimension 1
- v_cache: bfloat16 [2, 4096, 32, 4, 128], P(None, 'dp', None, 'tp'), parts along dimension 1
Outputs:
- output: bfloat16 [4096, 3584], P('dp'), parts along dimension 0
There are 4 independent parts. The reference program is written for one: setup_inputs(seed, part) draws one part's arguments, and reference() takes and returns one part's arrays. A program takes and returns all parts, laid end to end along the dimension named above; an argument that names none is the same for every part.
All inputs are finite; a program needn't handle non-finite values.
Results may differ from the reference program's by a relative error of at most 0.0165402.
Values are sent between devices in bfloat16 or wider.
A program may use at most 1.25 GiB of HBM per device.

```python
import math
import jax
import jax.numpy as jnp
from jax import lax

D = 3584
HEADS = 28
KV_HEADS = 4
FF = 18944
HEAD = 128
BATCH = 1024
SEQ = 32
LAYERS = 2
ROPE_BASE = 500000
NORM_EPS = 1e-5
GROUP = HEADS // KV_HEADS
LOG_LEVELS = int(math.log2(SEQ)) + 1


def draw_lengths(len_key):
    exp_key, val_key, top_key = jax.random.split(len_key, 3)
    span_exp = jax.random.randint(exp_key, (BATCH,), 0, LOG_LEVELS)
    span_limit = jnp.minimum(jnp.left_shift(jnp.ones_like(span_exp), span_exp), SEQ - 1)
    drawn_len = 1 + jax.random.randint(val_key, (BATCH,), 0, span_limit)
    full_slot = jax.random.randint(top_key, (), 0, BATCH)
    return jnp.where(jnp.arange(BATCH) == full_slot, SEQ - 1, drawn_len).astype(jnp.int32)


def setup_inputs(seed: int = 0, part: int = 0) -> dict:
    base_key = jax.random.key(seed)
    shared_keys = jax.random.split(base_key, 8)
    own_keys = jax.random.split(jax.random.fold_in(base_key, part), 4)
    q_width = HEADS * HEAD
    kv_width = KV_HEADS * HEAD

    def draw_weight(key_index, arr_shape, std_scale):
        return (jax.random.normal(shared_keys[key_index], arr_shape, jnp.float32) * std_scale).astype(jnp.bfloat16)

    return {
        'x_in': jax.random.normal(own_keys[0], (BATCH, D), jnp.float32).astype(jnp.bfloat16),
        'lengths': draw_lengths(own_keys[1]),
        'norm_gain': (1.0 + 0.3 * jax.random.normal(shared_keys[0], (LAYERS, D), jnp.float32)).astype(jnp.bfloat16),
        'w_q': draw_weight(1, (LAYERS, D, q_width), D ** -0.5),
        'w_k': draw_weight(2, (LAYERS, D, kv_width), 2.0 * D ** -0.5),
        'w_v': draw_weight(3, (LAYERS, D, kv_width), D ** -0.5),
        'w_o': draw_weight(4, (LAYERS, q_width, D), 2.0 * q_width ** -0.5),
        'w_gate': draw_weight(5, (LAYERS, D, FF), D ** -0.5),
        'w_up': draw_weight(6, (LAYERS, D, FF), D ** -0.5),
        'w_down': draw_weight(7, (LAYERS, FF, D), FF ** -0.5),
        'k_cache': (2.0 * jax.random.normal(own_keys[2], (LAYERS, BATCH, SEQ, KV_HEADS, HEAD), jnp.float32)).astype(jnp.bfloat16),
        'v_cache': jax.random.normal(own_keys[3], (LAYERS, BATCH, SEQ, KV_HEADS, HEAD), jnp.float32).astype(jnp.bfloat16),
    }


def rms_norm(x_res, gain_row):
    x_f32 = x_res.astype(jnp.float32)
    inv_rms = lax.rsqrt(jnp.mean(x_f32 * x_f32, axis=-1, keepdims=True) + NORM_EPS)
    return (x_f32 * inv_rms * gain_row.astype(jnp.float32)).astype(jnp.bfloat16)


def rope_rotate(head_vecs, positions):
    half_dim = HEAD // 2
    inv_freq = 1.0 / (ROPE_BASE ** (jnp.arange(0, HEAD, 2).astype(jnp.float32) / HEAD))
    angles = positions.astype(jnp.float32)[:, None] * inv_freq[None, :]
    cos_ang = jnp.cos(angles)[:, None, :]
    sin_ang = jnp.sin(angles)[:, None, :]
    vec_f32 = head_vecs.astype(jnp.float32)
    rot_first = vec_f32[..., :half_dim]
    rot_second = vec_f32[..., half_dim:]
    return jnp.concatenate([rot_first * cos_ang - rot_second * sin_ang, rot_second * cos_ang + rot_first * sin_ang], axis=-1).astype(jnp.bfloat16)


def decode_attention(q_rot, k_rot, v_new, k_layer, v_layer, lengths):
    attn_scale = HEAD ** -0.5
    q_f32 = q_rot.astype(jnp.float32)
    cache_logits = jnp.einsum('bkgd,bskd->bkgs', q_f32, k_layer.astype(jnp.float32)) * attn_scale
    valid_mask = jnp.arange(SEQ)[None, :] < lengths[:, None]
    cache_logits = jnp.where(valid_mask[:, None, None, :], cache_logits, -jnp.inf)
    self_logit = jnp.einsum('bkgd,bkd->bkg', q_f32, k_rot.astype(jnp.float32)) * attn_scale
    row_peak = jnp.maximum(jnp.max(cache_logits, axis=-1), self_logit)
    cache_w = jnp.exp(cache_logits - row_peak[..., None])
    self_w = jnp.exp(self_logit - row_peak)
    prob_denom = jnp.sum(cache_w, axis=-1) + self_w
    cache_p = (cache_w / prob_denom[..., None]).astype(jnp.bfloat16)
    self_p = (self_w / prob_denom).astype(jnp.bfloat16)
    cache_part = jnp.einsum('bkgs,bskd->bkgd', cache_p.astype(jnp.float32), v_layer.astype(jnp.float32))
    self_part = self_p.astype(jnp.float32)[..., None] * v_new.astype(jnp.float32)[:, :, None, :]
    return (cache_part + self_part).astype(jnp.bfloat16)


def reference(x_in, lengths, norm_gain, w_q, w_k, w_v, w_o, w_gate, w_up, w_down, k_cache, v_cache):
    def layer_step(x_res, layer_args):
        gain_row, wq_layer, wk_layer, wv_layer, wo_layer, wg_layer, wu_layer, wd_layer, k_layer, v_layer = layer_args
        normed = rms_norm(x_res, gain_row)
        q_proj = jnp.dot(normed, wq_layer, preferred_element_type=jnp.float32).astype(jnp.bfloat16).reshape(BATCH, HEADS, HEAD)
        k_proj = jnp.dot(normed, wk_layer, preferred_element_type=jnp.float32).astype(jnp.bfloat16).reshape(BATCH, KV_HEADS, HEAD)
        v_new = jnp.dot(normed, wv_layer, preferred_element_type=jnp.float32).astype(jnp.bfloat16).reshape(BATCH, KV_HEADS, HEAD)
        q_rot = rope_rotate(q_proj, lengths).reshape(BATCH, KV_HEADS, GROUP, HEAD)
        k_rot = rope_rotate(k_proj, lengths)
        attn_flat = decode_attention(q_rot, k_rot, v_new, k_layer, v_layer, lengths).reshape(BATCH, HEADS * HEAD)
        attn_proj = jnp.dot(attn_flat, wo_layer, preferred_element_type=jnp.float32)
        gate_act = jnp.dot(normed, wg_layer, preferred_element_type=jnp.float32).astype(jnp.bfloat16)
        up_act = jnp.dot(normed, wu_layer, preferred_element_type=jnp.float32).astype(jnp.bfloat16)
        mlp_hidden = (jax.nn.silu(gate_act.astype(jnp.float32)) * up_act.astype(jnp.float32)).astype(jnp.bfloat16)
        mlp_proj = jnp.dot(mlp_hidden, wd_layer, preferred_element_type=jnp.float32)
        x_next = (x_res.astype(jnp.float32) + attn_proj + mlp_proj).astype(jnp.bfloat16)
        return x_next, None

    scan_result = lax.scan(layer_step, x_in, (norm_gain, w_q, w_k, w_v, w_o, w_gate, w_up, w_down, k_cache, v_cache))
    return scan_result[0]
```

```python
import functools

import jax
import jax.numpy as jnp
from jax import lax
from jax.experimental import pallas as pl
from jax.experimental.pallas import tpu as pltpu
from jax.sharding import PartitionSpec as P

NORM_EPS = 1e-5
ROPE_BASE = 500000.0
MESH = pl.DeviceIdType.MESH
F32 = jnp.float32
BF16 = jnp.bfloat16

CHUNKS = 2
GU_TILE = 512
DN_TILE = 512
SUB = 256
KV_TOK = 64
GRP = 16
ROWS = 16
HOOK_SUM = 5
HOOK_FWD = 2


def layers_kernel(tp, dims, *refs):
    (x_in, lens, cos_t, sin_t, gain, wq, wk, wv, wo, wg, wu, wd, kc, vc, out,
     act, w1, wsp, w2, hid, qk, vnew, kbuf, vbuf, share, recv, xres,
     w1_sem, wsp_sem, w2_sem, kv_sem, io_sem, rs_send, rs_recv, ag_send, ag_recv) = refs
    L, tok, D, QW, HD, FF, SEQ = dims
    M = tok // CHUNKS
    Q = M // tp
    NH = QW // HD
    iters = L * CHUNKS
    GU_N = FF // GU_TILE
    REM = FF - GU_N * GU_TILE
    DN_N = D // DN_TILE
    KV_N = M // KV_TOK

    me = lax.axis_index("tp")
    half = me // 2
    low = me - half * 2
    sib = half * 2 + (1 - low)
    cross = (1 - half) * 2 + low
    diag = (1 - half) * 2 + (1 - low)
    peers = (sib, cross, diag)
    my_rows = pl.ds(pl.multiple_of(me * Q, Q), Q)

    def rows_of(dev):
        return pl.ds(pl.multiple_of(dev * Q, Q), Q)

    def qk_copies(l):
        return [pltpu.make_async_copy(wq.at[l], w1.at[0, :, pl.ds(0, QW)], w1_sem.at[0, 0]),
                pltpu.make_async_copy(wk.at[l], w1.at[0, :, pl.ds(QW, HD)], w1_sem.at[0, 1])]

    def gu_copies(l, j, slot):
        cols = pl.ds(pl.multiple_of(j * GU_TILE, GU_TILE), GU_TILE)
        return [pltpu.make_async_copy(wg.at[l, :, cols], w1.at[slot, :, pl.ds(0, GU_TILE)], w1_sem.at[slot, 0]),
                pltpu.make_async_copy(wu.at[l, :, cols], w1.at[slot, :, pl.ds(GU_TILE, GU_TILE)], w1_sem.at[slot, 1])]

    def sp_copies(l):
        rem = pl.ds(GU_N * GU_TILE, REM)
        return [pltpu.make_async_copy(wv.at[l], wsp.at[:, pl.ds(0, HD)], wsp_sem.at[0]),
                pltpu.make_async_copy(wg.at[l, :, rem], wsp.at[:, pl.ds(HD, REM)], wsp_sem.at[1]),
                pltpu.make_async_copy(wu.at[l, :, rem], wsp.at[:, pl.ds(HD + REM, REM)], wsp_sem.at[2])]

    def dn_copies(l, j, slot):
        cols = pl.ds(pl.multiple_of(j * DN_TILE, DN_TILE), DN_TILE)
        return [pltpu.make_async_copy(wo.at[l, :, cols], w2.at[slot, pl.ds(0, QW)], w2_sem.at[slot, 0]),
                pltpu.make_async_copy(wd.at[l, :, cols], w2.at[slot, pl.ds(QW, FF)], w2_sem.at[slot, 1])]

    def kv_copies(l, c, b, slot):
        toks = pl.ds(pl.multiple_of(c * M + b * KV_TOK, KV_TOK), KV_TOK)
        return [pltpu.make_async_copy(kc.at[l, toks], kbuf.at[slot], kv_sem.at[slot, 0]),
                pltpu.make_async_copy(vc.at[l, toks], vbuf.at[slot], kv_sem.at[slot, 1])]

    def start(copies):
        for cp in copies:
            cp.start()

    def wait(copies):
        for cp in copies:
            cp.wait()

    def share_copy(c, k, j):
        cols = pl.ds(pl.multiple_of(j * DN_TILE, DN_TILE), DN_TILE)
        return pltpu.make_async_remote_copy(
            src_ref=share.at[rows_of(peers[k]), cols], dst_ref=recv.at[c, k, :, cols],
            send_sem=rs_send.at[k], recv_sem=rs_recv.at[c, k],
            device_id={"tp": peers[k]}, device_id_type=MESH)

    def share_all(c, k):
        return pltpu.make_async_remote_copy(
            src_ref=share.at[rows_of(peers[k])], dst_ref=recv.at[c, k],
            send_sem=rs_send.at[k], recv_sem=rs_recv.at[c, k],
            device_id={"tp": peers[k]}, device_id_type=MESH)

    def gather_copy(c, k):
        block = rows_of(cross) if k == 2 else my_rows
        to = cross if k == 1 else sib
        return pltpu.make_async_remote_copy(
            src_ref=act.at[c, block], dst_ref=act.at[c, block],
            send_sem=ag_send.at[c, k], recv_sem=ag_recv.at[c, k],
            device_id={"tp": to}, device_id_type=MESH)

    def normed(xf, grow):
        inv = lax.rsqrt(jnp.mean(xf * xf, axis=-1, keepdims=True) + NORM_EPS)
        return (xf * inv * grow).astype(BF16)

    def sum_and_send(l, c):
        for k in range(3):
            share_all(c, k).wait_recv()
        last = l == L - 1
        grow = gain[jnp.minimum(l + 1, L - 1)]

        def step(r, carry):
            rr = pl.ds(pl.multiple_of(r * ROWS, ROWS), ROWS)
            own = pl.ds(pl.multiple_of(me * Q + r * ROWS, ROWS), ROWS)
            s = share[own, :].astype(F32)
            for k in range(3):
                s = s + recv[c, k, rr, :].astype(F32)
            xn = (xres[c, rr, :].astype(F32) + s).astype(BF16)
            xres[c, rr, :] = xn

            @pl.when(last)
            def _():
                act[c, own, :] = xn

            @pl.when(jnp.logical_not(last))
            def _():
                act[c, own, :] = normed(xn.astype(F32), grow)
            return carry

        lax.fori_loop(0, Q // ROWS, step, 0)
        gather_copy(c, 1).start()
        gather_copy(c, 0).start()

    def forward(c):
        gather_copy(c, 1).wait_recv()
        gather_copy(c, 2).start()

    def gathered(c):
        gather_copy(c, 0).wait_recv()
        gather_copy(c, 2).wait_recv()
        for k in range(3):
            gather_copy(c, k).wait_send()

    x_copies = [pltpu.make_async_copy(x_in.at[pl.ds(c * M, M)], act.at[c], io_sem.at[c]) for c in range(CHUNKS)]
    res_copies = [pltpu.make_async_copy(x_in.at[pl.ds(pl.multiple_of(c * M + me * Q, Q), Q)], xres.at[c], io_sem.at[CHUNKS + c])
                  for c in range(CHUNKS)]
    x_copies[0].start()
    start(qk_copies(0))
    start(sp_copies(0))
    start(kv_copies(0, 0, 0, 0))
    start(x_copies[1:])
    start(res_copies)

    barrier = pltpu.get_barrier_semaphore()
    for p in peers:
        pl.semaphore_signal(barrier, inc=1, device_id={"tp": p}, device_id_type=MESH)
    pl.semaphore_wait(barrier, 3)

    grow0 = gain[0]

    def first_norm(c):
        x_copies[c].wait()

        def step(r, carry):
            rr = pl.ds(pl.multiple_of(r * ROWS, ROWS), ROWS)
            act[c, rr, :] = normed(act[c, rr, :].astype(F32), grow0)
            return carry

        lax.fori_loop(0, M // ROWS, step, 0)

    first_norm(0)
    wait(res_copies)

    lane = lax.broadcasted_iota(jnp.int32, (GRP, 128), 1)
    trow = lax.broadcasted_iota(jnp.int32, (GRP, 128), 0)
    pos = lane % SEQ
    quad = 128 // SEQ
    in_group = (lane // SEQ) == (trow % quad)
    tgrp = trow // quad
    NG = GRP // quad
    scale = HD ** -0.5

    def attend(c, b, slot):
        for g in range(KV_TOK // GRP):
            r0 = pl.multiple_of(b * KV_TOK + g * GRP, GRP)
            rr = pl.ds(r0, GRP)
            tr = pl.ds(pl.multiple_of(c * M + b * KV_TOK + g * GRP, GRP), GRP)
            co, si = cos_t[tr, :], sin_t[tr, :]
            ok = jnp.logical_and(in_group, pos < lens[tr, :])

            def rot(z):
                zf = z.astype(F32)
                return (zf * co + pltpu.roll(zf, HD // 2, 1) * si).astype(BF16)

            kr = rot(qk[rr, pl.ds(QW, HD)]).astype(F32)
            qs = jnp.concatenate([rot(qk[rr, pl.ds(h * HD, HD)]) for h in range(NH)], axis=0)
            vn = vnew[rr, :].astype(F32)
            kb = kbuf[slot, pl.ds(g * GRP, GRP)].reshape(GRP * SEQ, HD)
            vb = vbuf[slot, pl.ds(g * GRP, GRP)].reshape(GRP * SEQ, HD)
            s = lax.dot_general(qs, kb, (((1,), (1,)), ((), ())), preferred_element_type=F32)
            s = s.reshape(NH, GRP, GRP * SEQ)
            lg = s[:, :, 0:128]
            for n in range(1, NG):
                lg = jnp.where((tgrp == n)[None], s[:, :, n * 128:(n + 1) * 128], lg)
            lg = jnp.where(ok[None], lg * scale, -jnp.inf)
            self_l = jnp.sum(qs.reshape(NH, GRP, HD).astype(F32) * kr[None], axis=-1, keepdims=True) * scale
            peak = jnp.maximum(jnp.max(lg, axis=-1, keepdims=True), self_l)
            w = jnp.exp(lg - peak)
            ws = jnp.exp(self_l - peak)
            den = jnp.sum(w, axis=-1, keepdims=True) + ws
            p = w / den
            ps = (ws / den).astype(BF16).astype(F32)
            pe = jnp.concatenate([jnp.where((tgrp == n)[None], p, 0.0) for n in range(NG)], axis=-1)
            pe = pe.astype(BF16).reshape(NH * GRP, GRP * SEQ)
            o = jnp.dot(pe, vb, preferred_element_type=F32).reshape(NH, GRP, HD)
            o = (o + ps * vn[None]).astype(BF16)
            for h in range(NH):
                hid[rr, pl.ds(h * HD, HD)] = o[h]

    def glu(gate, up):
        gf = gate.astype(BF16).astype(F32)
        uf = up.astype(BF16).astype(F32)
        return (gf * jax.nn.sigmoid(gf) * uf).astype(BF16)

    def dot(a, b):
        return jnp.dot(a, b, preferred_element_type=F32)

    def body(it, carry):
        l = it // CHUNKS
        c = it % CHUNKS
        pc = (it + CHUNKS - 1) % CHUNKS
        plr = (it + CHUNKS - 1) // CHUNKS - 1
        nl = (it + 1) // CHUNKS
        nc = (it + 1) % CHUNKS

        @pl.when(it == 1)
        def _():
            first_norm(1)

        @pl.when(it >= CHUNKS)
        def _():
            gathered(c)

        start(dn_copies(l, 0, 0))
        wait(qk_copies(l))
        start(gu_copies(l, 0, 1))
        for n in range((QW + HD) // SUB):
            qk[:, pl.ds(n * SUB, SUB)] = dot(act[c], w1[0, :, pl.ds(n * SUB, SUB)]).astype(BF16)
        wait(sp_copies(l))
        r = dot(act[c], wsp[...])
        vnew[...] = r[:, :HD].astype(BF16)
        hid[:, pl.ds(QW + GU_N * GU_TILE, REM)] = glu(r[:, HD:HD + REM], r[:, HD + REM:])
        start(dn_copies(l, 1, 1))

        def att_step(b, carry):
            slot = b % 2

            @pl.when(b + 1 < KV_N)
            def _():
                start(kv_copies(l, c, b + 1, 1 - slot))

            wait(kv_copies(l, c, b, slot))
            attend(c, b, slot)
            return carry

        lax.fori_loop(0, KV_N, att_step, 0)

        def gu_step(j, carry):
            slot = (j + 1) % 2

            @pl.when(j + 1 < GU_N)
            def _():
                start(gu_copies(l, j + 1, 1 - slot))

            @pl.when(jnp.logical_and(j + 1 == GU_N, it + 1 < iters))
            def _():
                start(qk_copies(nl))
                start(sp_copies(nl))
                start(kv_copies(nl, nc, 0, 0))

            @pl.when(jnp.logical_and(j == HOOK_SUM, it > 0))
            def _():
                sum_and_send(plr, pc)

            wait(gu_copies(l, j, slot))
            for n in range(GU_TILE // SUB):
                g = dot(act[c], w1[slot, :, pl.ds(n * SUB, SUB)])
                u = dot(act[c], w1[slot, :, pl.ds(GU_TILE + n * SUB, SUB)])
                hid[:, pl.ds(pl.multiple_of(QW + j * GU_TILE + n * SUB, 128), SUB)] = glu(g, u)
            return carry

        lax.fori_loop(0, GU_N, gu_step, 0)

        @pl.when(it > 0)
        def _():
            for k in range(3):
                share_all(pc, k).wait_send()

        def dn_step(j, carry):
            slot = j % 2

            @pl.when(jnp.logical_and(j == HOOK_FWD, it > 0))
            def _():
                forward(pc)

            wait(dn_copies(l, j, slot))

            @pl.when(j > 0)
            def _():
                for k in (1, 2, 0):
                    share_copy(c, k, j - 1).start()

            for n in range(DN_TILE // SUB):
                share[:, pl.ds(pl.multiple_of(j * DN_TILE + n * SUB, SUB), SUB)] = dot(
                    hid[...], w2[slot, :, pl.ds(n * SUB, SUB)]).astype(BF16)

            @pl.when(j + 2 < DN_N)
            def _():
                start(dn_copies(l, j + 2, slot))
            return carry

        lax.fori_loop(0, DN_N, dn_step, 0)
        for k in (1, 2, 0):
            share_copy(c, k, DN_N - 1).start()
        return carry

    lax.fori_loop(0, iters, body, 0)

    fc = (iters - 1) % CHUNKS
    outs = []
    for c in [(iters - CHUNKS + i) % CHUNKS for i in range(CHUNKS)]:
        if c == fc:
            sum_and_send(jnp.int32(L - 1), fc)
            for k in range(3):
                share_all(fc, k).wait_send()
            forward(fc)
        gathered(c)
        cp = pltpu.make_async_copy(act.at[c], out.at[pl.ds(c * M, M)], io_sem.at[c])
        cp.start()
        outs.append(cp)
    wait(outs)


def solution(mesh):
    tp_size = mesh.shape['tp']
    arg_specs = (P('dp', None), P('dp'), P(), P(None, None, 'tp'), P(None, None, 'tp'), P(None, None, 'tp'), P(None, 'tp', None), P(None, None, 'tp'), P(None, None, 'tp'), P(None, 'tp', None), P(None, 'dp', None, 'tp', None), P(None, 'dp', None, 'tp', None))

    def per_device(x_in, lengths, norm_gain, w_q, w_k, w_v, w_o, w_gate, w_up, w_down, k_cache, v_cache):
        L, tok, seq, kvh, hd = k_cache.shape
        D = x_in.shape[1]
        qw = w_q.shape[2]
        ff = w_gate.shape[2]
        inv_freq = 1.0 / (ROPE_BASE ** (jnp.arange(0, hd, 2).astype(F32) / hd))
        ang = lengths.astype(F32)[:, None] * inv_freq[None, :]
        cos, sin = jnp.cos(ang), jnp.sin(ang)
        cos_t = jnp.concatenate([cos, cos], axis=-1)
        sin_t = jnp.concatenate([-sin, sin], axis=-1)
        lens = jnp.broadcast_to(lengths[:, None], (tok, 128))
        kc = k_cache.reshape(L, tok, seq, hd)
        vc = v_cache.reshape(L, tok, seq, hd)
        M = tok // CHUNKS
        Q = M // tp_size
        vmem = pl.BlockSpec(memory_space=pltpu.VMEM)
        hbm = pl.BlockSpec(memory_space=pl.ANY)
        dma = pltpu.SemaphoreType.DMA
        rem = ff - (ff // GU_TILE) * GU_TILE
        return pl.pallas_call(
            functools.partial(layers_kernel, tp_size, (L, tok, D, qw, hd, ff, seq)),
            out_shape=jax.ShapeDtypeStruct((tok, D), BF16),
            in_specs=[hbm, vmem, vmem, vmem, vmem] + [hbm] * 9,
            out_specs=hbm,
            scratch_shapes=[
                pltpu.VMEM((CHUNKS, M, D), BF16),
                pltpu.VMEM((2, D, 2 * GU_TILE), BF16),
                pltpu.VMEM((D, hd + 2 * rem), BF16),
                pltpu.VMEM((2, qw + ff, DN_TILE), BF16),
                pltpu.VMEM((M, qw + ff), BF16),
                pltpu.VMEM((M, qw + hd), BF16),
                pltpu.VMEM((M, hd), BF16),
                pltpu.VMEM((2, KV_TOK, seq, hd), BF16),
                pltpu.VMEM((2, KV_TOK, seq, hd), BF16),
                pltpu.VMEM((M, D), BF16),
                pltpu.VMEM((CHUNKS, 3, Q, D), BF16),
                pltpu.VMEM((CHUNKS, Q, D), BF16),
                dma((2, 2)), dma((3,)), dma((2, 2)), dma((2, 2)), dma((2 * CHUNKS,)),
                dma((3,)), dma((CHUNKS, 3)), dma((CHUNKS, 3)), dma((CHUNKS, 3)),
            ],
            compiler_params=pltpu.CompilerParams(
                collective_id=0, has_side_effects=True, vmem_limit_bytes=67043328),
            name="layers",
        )(x_in, lens, cos_t, sin_t, norm_gain.astype(F32).reshape(L, 1, D), w_q, w_k, w_v, w_o, w_gate, w_up, w_down, kc, vc)

    return jax.shard_map(per_device, mesh=mesh, in_specs=arg_specs, out_specs=P('dp', None), check_vma=False)
```

```python
import functools

import jax
import jax.numpy as jnp
from jax import lax
from jax.experimental import pallas as pl
from jax.experimental.pallas import tpu as pltpu
from jax.sharding import PartitionSpec as P

NORM_EPS = 1e-5
ROPE_BASE = 500000.0
MESH = pl.DeviceIdType.MESH
F32 = jnp.float32
BF16 = jnp.bfloat16

CHUNKS = 2
GU_TILE = 512
DN_TILE = 512
SUB = 256
KV_TOK = 64
GRP = 16
ROWS = 16
UNROLL = 2
HOOK_SUM = 5
HOOK_FWD = 3


def layers_kernel(tp, dims, *refs):
    (x_in, lens, cs_t, gain, wq, wk, wv, wo, wg, wu, wd, kc, vc, out,
     act, w1, wsp, w2, hid, qk, vnew, kbuf, vbuf, share, recv, xres, logit, selfp, prob,
     w1_sem, wsp_sem, w2_sem, kv_sem, io_sem, rs_send, rs_recv, ag_send, ag_recv, fin_send, fin_recv) = refs
    L, tok, D, QW, HD, FF, SEQ = dims
    M = tok // CHUNKS
    Q = M // tp
    NH = QW // HD
    iters = L * CHUNKS
    GU_N = FF // GU_TILE
    REM = FF - GU_N * GU_TILE
    DN_N = D // DN_TILE
    PIECES = D // SUB
    PER = DN_TILE // SUB
    KV_N = M // KV_TOK

    me = lax.axis_index("tp")
    half = me // 2
    low = me - half * 2
    sib = half * 2 + (1 - low)
    cross = (1 - half) * 2 + low
    diag = (1 - half) * 2 + (1 - low)
    peers = (sib, cross, diag)
    my_rows = pl.ds(pl.multiple_of(me * Q, Q), Q)

    def rows_of(dev):
        return pl.ds(pl.multiple_of(dev * Q, Q), Q)

    def qk_copies(l):
        return [pltpu.make_async_copy(wq.at[l], w1.at[0, :, pl.ds(0, QW)], w1_sem.at[0, 0]),
                pltpu.make_async_copy(wk.at[l], w1.at[0, :, pl.ds(QW, HD)], w1_sem.at[0, 1])]

    def gu_copies(l, j, slot):
        cols = pl.ds(pl.multiple_of(j * GU_TILE, GU_TILE), GU_TILE)
        return [pltpu.make_async_copy(wg.at[l, :, cols], w1.at[slot, :, pl.ds(0, GU_TILE)], w1_sem.at[slot, 0]),
                pltpu.make_async_copy(wu.at[l, :, cols], w1.at[slot, :, pl.ds(GU_TILE, GU_TILE)], w1_sem.at[slot, 1])]

    def sp_copies(l):
        rem = pl.ds(GU_N * GU_TILE, REM)
        return [pltpu.make_async_copy(wv.at[l], wsp.at[:, pl.ds(0, HD)], wsp_sem.at[0]),
                pltpu.make_async_copy(wg.at[l, :, rem], wsp.at[:, pl.ds(HD, REM)], wsp_sem.at[1]),
                pltpu.make_async_copy(wu.at[l, :, rem], wsp.at[:, pl.ds(HD + REM, REM)], wsp_sem.at[2])]

    def dn_copies(l, j, slot):
        cols = pl.ds(pl.multiple_of(j * DN_TILE, DN_TILE), DN_TILE)
        return [pltpu.make_async_copy(wo.at[l, :, cols], w2.at[slot, pl.ds(0, QW)], w2_sem.at[slot, 0]),
                pltpu.make_async_copy(wd.at[l, :, cols], w2.at[slot, pl.ds(QW, FF)], w2_sem.at[slot, 1])]

    def kv_copies(l, c, b, slot):
        toks = pl.ds(pl.multiple_of(c * M + b * KV_TOK, KV_TOK), KV_TOK)
        return [pltpu.make_async_copy(kc.at[l, toks], kbuf.at[slot], kv_sem.at[slot, 0]),
                pltpu.make_async_copy(vc.at[l, toks], vbuf.at[slot], kv_sem.at[slot, 1])]

    def start(copies):
        for cp in copies:
            cp.start()

    def wait(copies):
        for cp in copies:
            cp.wait()

    def piece(p):
        return pl.ds(pl.multiple_of(p * SUB, SUB), SUB)

    def share_copy(c, k, j):
        cols = piece(j)
        return pltpu.make_async_remote_copy(
            src_ref=share.at[rows_of(peers[k]), cols], dst_ref=recv.at[c, k, :, cols],
            send_sem=rs_send.at[k], recv_sem=rs_recv.at[c, k, j],
            device_id={"tp": peers[k]}, device_id_type=MESH)

    def send_piece(c, j):
        for k in (1, 2, 0):
            share_copy(c, k, j).start()

    def share_all(c, k):
        return pltpu.make_async_remote_copy(
            src_ref=share.at[rows_of(peers[k])], dst_ref=recv.at[c, k],
            send_sem=rs_send.at[k], recv_sem=rs_recv.at[c, k, 0],
            device_id={"tp": peers[k]}, device_id_type=MESH)

    def gather_copy(c, k):
        block = rows_of(cross) if k == 2 else my_rows
        to = cross if k == 1 else sib
        return pltpu.make_async_remote_copy(
            src_ref=act.at[c, block], dst_ref=act.at[c, block],
            send_sem=ag_send.at[c, k], recv_sem=ag_recv.at[c, k],
            device_id={"tp": to}, device_id_type=MESH)

    def gain_row(l):
        rows = gain[...].astype(F32)
        row = rows[0:1]
        for i in range(1, L):
            row = jnp.where(l >= i, rows[i:i + 1], row)
        return row

    def normed(xf, grow):
        inv = lax.rsqrt(jnp.mean(xf * xf, axis=-1, keepdims=True) + NORM_EPS)
        return xf * inv * grow

    def groups_of(r, base):
        return [pl.ds(pl.multiple_of(base + (r * UNROLL + i) * ROWS, ROWS), ROWS) for i in range(UNROLL)]

    def sum_and_send(l, c):
        def arrived(j, carry):
            for k in range(3):
                share_copy(c, k, j).wait_recv()
            return carry

        lax.fori_loop(0, PIECES, arrived, 0)
        last = l == L - 1
        grow = gain_row(l + 1)

        def step(r, carry):
            rows, owns = groups_of(r, 0), groups_of(r, me * Q)
            new = []
            for rr, own in zip(rows, owns):
                s = share[own, :].astype(F32)
                for k in range(3):
                    s = s + recv[c, k, rr, :].astype(F32)
                xn = (xres[c, rr, :].astype(F32) + s).astype(BF16)
                xf = xn.astype(F32)
                new.append((xn, jnp.where(last, xf, normed(xf, grow)).astype(BF16)))
            for rr, own, (xn, a) in zip(rows, owns, new):
                xres[c, rr, :] = xn
                act[c, own, :] = a
            return carry

        lax.fori_loop(0, Q // (ROWS * UNROLL), step, 0)
        gather_copy(c, 1).start()
        gather_copy(c, 0).start()

    def forward(c):
        gather_copy(c, 1).wait_recv()
        gather_copy(c, 2).start()

    def gathered(c):
        gather_copy(c, 0).wait_recv()
        gather_copy(c, 2).wait_recv()
        for k in range(3):
            gather_copy(c, k).wait_send()

    x_copies = [pltpu.make_async_copy(x_in.at[pl.ds(c * M, M)], act.at[c], io_sem.at[c]) for c in range(CHUNKS)]
    res_copies = [pltpu.make_async_copy(x_in.at[pl.ds(pl.multiple_of(c * M + me * Q, Q), Q)], xres.at[c], io_sem.at[CHUNKS + c])
                  for c in range(CHUNKS)]
    x_copies[0].start()
    start(qk_copies(0))
    start(sp_copies(0))
    start(kv_copies(0, 0, 0, 0))
    start(x_copies[1:])
    start(res_copies)

    barrier = pltpu.get_barrier_semaphore()
    for p in peers:
        pl.semaphore_signal(barrier, inc=1, device_id={"tp": p}, device_id_type=MESH)
    pl.semaphore_wait(barrier, 3)

    grow0 = gain_row(0)

    def first_norm(c):
        x_copies[c].wait()

        def step(r, carry):
            rows = groups_of(r, 0)
            new = [normed(act[c, rr, :].astype(F32), grow0).astype(BF16) for rr in rows]
            for rr, a in zip(rows, new):
                act[c, rr, :] = a
            return carry

        lax.fori_loop(0, M // (ROWS * UNROLL), step, 0)

    first_norm(0)
    wait(res_copies)

    lane = lax.broadcasted_iota(jnp.int32, (GRP, 128), 1)
    trow = lax.broadcasted_iota(jnp.int32, (GRP, 128), 0)
    pos = lane % SEQ
    quad = 128 // SEQ
    in_group = (lane // SEQ) == (trow % quad)
    tgrp = trow // quad
    NG = GRP // quad
    scale = HD ** -0.5

    first_half = lane < HD // 2
    groups = range(KV_TOK // GRP)

    def toks(base, b, g):
        return pl.ds(pl.multiple_of(base + b * KV_TOK + g * GRP, GRP), GRP)

    def attend_scores(c, b, slot, g):
        rr, tr = toks(0, b, g), toks(c * M, b, g)
        cs = cs_t[tr, :]
        sc = pltpu.roll(cs, HD // 2, 1)
        co = jnp.where(first_half, cs, sc)
        si = jnp.where(first_half, -sc, cs)

        def rot(z):
            zf = z.astype(F32)
            return (zf * co + pltpu.roll(zf, HD // 2, 1) * si).astype(BF16)

        kr = rot(qk[rr, pl.ds(QW, HD)]).astype(F32)
        qs = jnp.concatenate([rot(qk[rr, pl.ds(h * HD, HD)]) for h in range(NH)], axis=0)
        kb = kbuf[slot, pl.ds(g * GRP, GRP)].reshape(GRP * SEQ, HD)
        s = lax.dot_general(qs, kb, (((1,), (1,)), ((), ())), preferred_element_type=F32)
        s = s.reshape(NH, GRP, GRP * SEQ)
        lg = s[:, :, 0:128]
        for n in range(1, NG):
            lg = jnp.where((tgrp == n)[None], s[:, :, n * 128:(n + 1) * 128], lg)
        ok = jnp.logical_and(in_group, pos < lens[tr, :])
        logit[g] = jnp.where(ok[None], lg * scale, -jnp.inf)
        selfl = jnp.sum(qs.reshape(NH, GRP, HD).astype(F32) * kr[None], axis=-1, keepdims=True) * scale
        selfp[g] = jnp.broadcast_to(selfl, (NH, GRP, HD))

    def attend_softmax(g):
        lg = logit[g]
        self_l = selfp[g]
        peak = jnp.maximum(jnp.max(lg, axis=-1, keepdims=True), self_l)
        w = jnp.exp(lg - peak)
        ws = jnp.exp(self_l - peak)
        den = jnp.sum(w, axis=-1, keepdims=True) + ws
        p = w / den
        selfp[g] = (ws / den).astype(BF16).astype(F32)
        pe = jnp.concatenate([jnp.where((tgrp == n)[None], p, 0.0) for n in range(NG)], axis=-1)
        prob[g] = pe.astype(BF16).reshape(NH * GRP, GRP * SEQ)

    def attend_values(b, slot, g):
        rr = toks(0, b, g)
        vb = vbuf[slot, pl.ds(g * GRP, GRP)].reshape(GRP * SEQ, HD)
        o = jnp.dot(prob[g], vb, preferred_element_type=F32).reshape(NH, GRP, HD)
        o = (o + selfp[g] * vnew[rr, :].astype(F32)[None]).astype(BF16)
        for h in range(NH):
            hid[rr, pl.ds(h * HD, HD)] = o[h]

    def glu(gate, up):
        gf = gate.astype(BF16).astype(F32)
        uf = up.astype(BF16).astype(F32)
        return (gf * jax.nn.sigmoid(gf) * uf).astype(BF16)

    def dot(a, b):
        return jnp.dot(a, b, preferred_element_type=F32)

    def body(it, carry):
        l = it // CHUNKS
        c = it % CHUNKS
        pc = (it + CHUNKS - 1) % CHUNKS
        plr = (it + CHUNKS - 1) // CHUNKS - 1
        nl = (it + 1) // CHUNKS
        nc = (it + 1) % CHUNKS

        @pl.when(it == 1)
        def _():
            first_norm(1)

        @pl.when(it >= CHUNKS)
        def _():
            gathered(c)

        start(dn_copies(l, 0, 0))
        wait(qk_copies(l))
        start(gu_copies(l, 0, 1))
        for n in range((QW + HD) // SUB):
            qk[:, pl.ds(n * SUB, SUB)] = dot(act[c], w1[0, :, pl.ds(n * SUB, SUB)]).astype(BF16)
        wait(sp_copies(l))
        r = dot(act[c], wsp[...])
        vnew[...] = r[:, :HD].astype(BF16)
        hid[:, pl.ds(QW + GU_N * GU_TILE, REM)] = glu(r[:, HD:HD + REM], r[:, HD + REM:])
        start(dn_copies(l, 1, 1))

        def gu_step(j, carry, attend):
            slot = (j + 1) % 2
            kvs = j % 2

            if attend:
                @pl.when(j + 1 < KV_N)
                def _():
                    start(kv_copies(l, c, j + 1, 1 - kvs))

            @pl.when(j + 1 < GU_N)
            def _():
                start(gu_copies(l, j + 1, 1 - slot))

            @pl.when(jnp.logical_and(j + 1 == GU_N, it + 1 < iters))
            def _():
                start(qk_copies(nl))
                start(sp_copies(nl))
                start(kv_copies(nl, nc, 0, 0))

            @pl.when(jnp.logical_and(j == HOOK_SUM, it > 0))
            def _():
                sum_and_send(plr, pc)

            wait(gu_copies(l, j, slot))
            if attend:
                wait(kv_copies(l, c, j, kvs))
            stages = [lambda g: attend_scores(c, j, kvs, g), attend_softmax, lambda g: attend_values(j, kvs, g)]
            for n in range(GU_TILE // SUB):
                gu = []
                for half_cols in (0, GU_TILE):
                    gu.append(dot(act[c], w1[slot, :, pl.ds(half_cols + n * SUB, SUB)]))
                    if attend and stages:
                        stage = stages.pop(0)
                        for g in groups:
                            stage(g)
                hid[:, pl.ds(pl.multiple_of(QW + j * GU_TILE + n * SUB, 128), SUB)] = glu(*gu)
            return carry

        lax.fori_loop(0, KV_N, functools.partial(gu_step, attend=True), 0)
        lax.fori_loop(KV_N, GU_N, functools.partial(gu_step, attend=False), 0)

        @pl.when(it > 0)
        def _():
            for k in range(3):
                share_all(pc, k).wait_send()

        def dn_step(j, carry):
            slot = j % 2

            @pl.when(jnp.logical_and(j == HOOK_FWD, it > 0))
            def _():
                forward(pc)

            wait(dn_copies(l, j, slot))

            for n in range(PER):
                share[:, pl.ds(pl.multiple_of(j * DN_TILE + n * SUB, SUB), SUB)] = dot(
                    hid[...], w2[slot, :, pl.ds(n * SUB, SUB)]).astype(BF16)

            @pl.when(j + 2 < DN_N)
            def _():
                start(dn_copies(l, j + 2, slot))

            @pl.when(j > 0)
            def _():
                send_piece(c, j * PER - 1)

            for n in range(PER - 1):
                send_piece(c, j * PER + n)
            return carry

        lax.fori_loop(0, DN_N, dn_step, 0)
        send_piece(c, PIECES - 1)
        return carry

    lax.fori_loop(0, iters, body, 0)

    fc = (iters - 1) % CHUNKS

    def final_copy(k, j):
        block = rows_of(cross) if k == 2 else my_rows
        return pltpu.make_async_remote_copy(
            src_ref=act.at[fc, block, piece(j)], dst_ref=act.at[fc, block, piece(j)],
            send_sem=fin_send.at[k], recv_sem=fin_recv.at[k, j],
            device_id={"tp": cross if k == 1 else sib}, device_id_type=MESH)

    def out_copy(j):
        return pltpu.make_async_copy(
            act.at[fc, :, piece(j)], out.at[pl.ds(fc * M, M), piece(j)], io_sem.at[fc])

    out_copies = []
    for c in range(CHUNKS):
        if c != fc:
            gathered(c)
            cp = pltpu.make_async_copy(act.at[c], out.at[pl.ds(c * M, M)], io_sem.at[c])
            cp.start()
            out_copies.append(cp)

    def final_sum(j, carry):
        for k in range(3):
            share_copy(fc, k, j).wait_recv()
        for r in range(0, Q, ROWS):
            own = pl.ds(pl.multiple_of(me * Q + r, ROWS), ROWS)
            t = share[own, piece(j)].astype(F32)
            for k in range(3):
                t = t + recv[fc, k, pl.ds(r, ROWS), piece(j)].astype(F32)
            act[fc, own, piece(j)] = (xres[fc, pl.ds(r, ROWS), piece(j)].astype(F32) + t).astype(BF16)
        final_copy(1, j).start()
        final_copy(0, j).start()
        return carry

    lax.fori_loop(0, PIECES, final_sum, 0)

    def final_forward(j, carry):
        @pl.when(j < PIECES)
        def _():
            final_copy(1, j).wait_recv()
            final_copy(2, j).start()

        @pl.when(j > 0)
        def _():
            final_copy(0, j - 1).wait_recv()
            final_copy(2, j - 1).wait_recv()
            out_copy(j - 1).start()
        return carry

    lax.fori_loop(0, PIECES + 1, final_forward, 0)
    for k in range(3):
        share_all(fc, k).wait_send()
        block = rows_of(cross) if k == 2 else my_rows
        pltpu.make_async_remote_copy(
            src_ref=act.at[fc, block], dst_ref=act.at[fc, block], send_sem=fin_send.at[k],
            recv_sem=fin_recv.at[k, 0], device_id={"tp": cross if k == 1 else sib},
            device_id_type=MESH).wait_send()
    pltpu.make_async_copy(act.at[fc], out.at[pl.ds(fc * M, M)], io_sem.at[fc]).wait()
    wait(out_copies)


def solution(mesh):
    tp_size = mesh.shape['tp']
    arg_specs = (P('dp', None), P('dp'), P(), P(None, None, 'tp'), P(None, None, 'tp'), P(None, None, 'tp'), P(None, 'tp', None), P(None, None, 'tp'), P(None, None, 'tp'), P(None, 'tp', None), P(None, 'dp', None, 'tp', None), P(None, 'dp', None, 'tp', None))

    def per_device(x_in, lengths, norm_gain, w_q, w_k, w_v, w_o, w_gate, w_up, w_down, k_cache, v_cache):
        L, tok, seq, kvh, hd = k_cache.shape
        D = x_in.shape[1]
        qw = w_q.shape[2]
        ff = w_gate.shape[2]
        inv_freq = 1.0 / (ROPE_BASE ** (jnp.arange(0, hd, 2).astype(F32) / hd))
        ang = lengths.astype(F32)[:, None] * inv_freq[None, :]
        cs_t = jnp.concatenate([jnp.cos(ang), jnp.sin(ang)], axis=-1)
        lens = jnp.broadcast_to(lengths[:, None], (tok, 128))
        kc = k_cache.reshape(L, tok, seq, hd)
        vc = v_cache.reshape(L, tok, seq, hd)
        M = tok // CHUNKS
        Q = M // tp_size
        vmem = pl.BlockSpec(memory_space=pltpu.VMEM)
        hbm = pl.BlockSpec(memory_space=pl.ANY)
        dma = pltpu.SemaphoreType.DMA
        rem = ff - (ff // GU_TILE) * GU_TILE
        return pl.pallas_call(
            functools.partial(layers_kernel, tp_size, (L, tok, D, qw, hd, ff, seq)),
            out_shape=jax.ShapeDtypeStruct((tok, D), BF16),
            in_specs=[hbm, vmem, vmem, vmem] + [hbm] * 9,
            out_specs=hbm,
            scratch_shapes=[
                pltpu.VMEM((CHUNKS, M, D), BF16),
                pltpu.VMEM((2, D, 2 * GU_TILE), BF16),
                pltpu.VMEM((D, hd + 2 * rem), BF16),
                pltpu.VMEM((2, qw + ff, DN_TILE), BF16),
                pltpu.VMEM((M, qw + ff), BF16),
                pltpu.VMEM((M, qw + hd), BF16),
                pltpu.VMEM((M, hd), BF16),
                pltpu.VMEM((2, KV_TOK, seq, hd), BF16),
                pltpu.VMEM((2, KV_TOK, seq, hd), BF16),
                pltpu.VMEM((M, D), BF16),
                pltpu.VMEM((CHUNKS, 3, Q, D), BF16),
                pltpu.VMEM((CHUNKS, Q, D), BF16),
                pltpu.VMEM((KV_TOK // GRP, qw // hd, GRP, hd), F32),
                pltpu.VMEM((KV_TOK // GRP, qw // hd, GRP, hd), F32),
                pltpu.VMEM((KV_TOK // GRP, qw // hd * GRP, GRP * seq), BF16),
                dma((2, 2)), dma((3,)), dma((2, 2)), dma((2, 2)), dma((2 * CHUNKS,)),
                dma((3,)), dma((CHUNKS, 3, D // SUB)), dma((CHUNKS, 3)), dma((CHUNKS, 3)),
                dma((3,)), dma((3, D // SUB)),
            ],
            compiler_params=pltpu.CompilerParams(
                collective_id=0, has_side_effects=True, vmem_limit_bytes=67043328),
            name="layers",
        )(x_in, lens, cs_t, norm_gain, w_q, w_k, w_v, w_o, w_gate, w_up, w_down, kc, vc)

    return jax.shard_map(per_device, mesh=mesh, in_specs=arg_specs, out_specs=P('dp', None), check_vma=False)
```

```python
import functools

import jax
import jax.numpy as jnp
from jax import lax
from jax.experimental import pallas as pl
from jax.experimental.pallas import tpu as pltpu
from jax.sharding import PartitionSpec as P

NORM_EPS = 1e-5
ROPE_BASE = 500000.0
MESH = pl.DeviceIdType.MESH
F32 = jnp.float32
BF16 = jnp.bfloat16

CHUNKS = 2
GU_TILE = 512
DN_TILE = 512
SUB = 256
KV_TOK = 64
GRP = 16
ROWS = 16
UNROLL = 2
HOOK_SUM = 5
HOOK_FWD = 3


def layers_kernel(tp, dims, *refs):
    (x_in, lens, cs_t, gain, wq, wk, wv, wo, wg, wu, wd, kc, vc, out, wx,
     act, w1, w2, hid, qk, vnew, kbuf, vbuf, share, recv, xres, logit, selfp, prob, hsib,
     w1_sem, wsp_sem, w2_sem, kv_sem, io_sem, rs_send, rs_recv, ag_send, ag_recv, fin_send, fin_recv,
     wx_sem, hx_sem, xx_sem) = refs
    L, tok, D, QW, HD, FF, SEQ = dims
    M = tok // CHUNKS
    Q = M // tp
    NH = QW // HD
    iters = L * CHUNKS
    GU_N = FF // GU_TILE
    REM = FF - GU_N * GU_TILE
    DN_N = D // DN_TILE
    PIECES = D // SUB
    PER = DN_TILE // SUB
    HC = D // 2
    HR = M // 2
    HP = HC // SUB
    WX_ROWS = 128
    WX_N = (QW + FF) // WX_ROWS
    WX_PER = -(-WX_N // ((iters - 1) * GU_N))
    KV_N = M // KV_TOK

    me = lax.axis_index("tp")
    half = me // 2
    low = me - half * 2
    sib = half * 2 + (1 - low)
    cross = (1 - half) * 2 + low
    diag = (1 - half) * 2 + (1 - low)
    peers = (sib, cross, diag)
    my_rows = pl.ds(pl.multiple_of(me * Q, Q), Q)

    def rows_of(dev):
        return pl.ds(pl.multiple_of(dev * Q, Q), Q)

    def qk_copies(l):
        return [pltpu.make_async_copy(wq.at[l], w1.at[0, :, pl.ds(0, QW)], w1_sem.at[0, 0]),
                pltpu.make_async_copy(wk.at[l], w1.at[0, :, pl.ds(QW, HD)], w1_sem.at[0, 1])]

    def gu_copies(l, j, slot):
        cols = pl.ds(pl.multiple_of(j * GU_TILE, GU_TILE), GU_TILE)
        return [pltpu.make_async_copy(wg.at[l, :, cols], w1.at[slot, :, pl.ds(0, GU_TILE)], w1_sem.at[slot, 0]),
                pltpu.make_async_copy(wu.at[l, :, cols], w1.at[slot, :, pl.ds(GU_TILE, GU_TILE)], w1_sem.at[slot, 1])]

    def sp_copies(l):
        rem = pl.ds(GU_N * GU_TILE, REM)
        return [pltpu.make_async_copy(wv.at[l], w1.at[1, :, pl.ds(0, HD)], wsp_sem.at[0]),
                pltpu.make_async_copy(wg.at[l, :, rem], w1.at[1, :, pl.ds(HD, REM)], wsp_sem.at[1]),
                pltpu.make_async_copy(wu.at[l, :, rem], w1.at[1, :, pl.ds(HD + REM, REM)], wsp_sem.at[2])]

    def dn_copies(l, j, slot):
        cols = pl.ds(pl.multiple_of(j * DN_TILE, DN_TILE), DN_TILE)
        return [pltpu.make_async_copy(wo.at[l, :, cols], w2.at[slot, pl.ds(0, QW)], w2_sem.at[slot, 0]),
                pltpu.make_async_copy(wd.at[l, :, cols], w2.at[slot, pl.ds(QW, FF)], w2_sem.at[slot, 1])]

    def half_cols(core, j):
        return pl.ds(pl.multiple_of(core * HC + j * SUB, SUB), SUB)

    def dn2_copies(j, slot):
        own, got = half_cols(low, j), pl.ds(pl.multiple_of(j * SUB, SUB), SUB)
        return [pltpu.make_async_copy(wo.at[L - 1, :, own], w2.at[slot, pl.ds(0, QW), pl.ds(0, SUB)], w2_sem.at[slot, 0]),
                pltpu.make_async_copy(wd.at[L - 1, :, own], w2.at[slot, pl.ds(QW, FF), pl.ds(0, SUB)], w2_sem.at[slot, 1]),
                pltpu.make_async_copy(wx.at[:, got], w2.at[slot, :, pl.ds(SUB, SUB)], w2_sem.at[slot, 2])]

    def kv_copies(l, c, b, slot):
        toks = pl.ds(pl.multiple_of(c * M + b * KV_TOK, KV_TOK), KV_TOK)
        return [pltpu.make_async_copy(kc.at[l, toks], kbuf.at[slot], kv_sem.at[slot, 0]),
                pltpu.make_async_copy(vc.at[l, toks], vbuf.at[slot], kv_sem.at[slot, 1])]

    def start(copies):
        for cp in copies:
            cp.start()

    def wait(copies):
        for cp in copies:
            cp.wait()

    def piece(p):
        return pl.ds(pl.multiple_of(p * SUB, SUB), SUB)

    def share_copy(c, k, j):
        cols = piece(j)
        return pltpu.make_async_remote_copy(
            src_ref=share.at[rows_of(peers[k]), cols], dst_ref=recv.at[c, k, :, cols],
            send_sem=rs_send.at[k], recv_sem=rs_recv.at[c, k, j],
            device_id={"tp": peers[k]}, device_id_type=MESH)

    def send_piece(c, j):
        for k in (1, 2, 0):
            share_copy(c, k, j).start()

    def share_all(c, k):
        return pltpu.make_async_remote_copy(
            src_ref=share.at[rows_of(peers[k])], dst_ref=recv.at[c, k],
            send_sem=rs_send.at[k], recv_sem=rs_recv.at[c, k, 0],
            device_id={"tp": peers[k]}, device_id_type=MESH)

    def to_sib(src, dst, sems):
        return pltpu.make_async_remote_copy(
            src_ref=src, dst_ref=dst, send_sem=sems.at[0], recv_sem=sems.at[1],
            device_id={"tp": sib}, device_id_type=MESH)

    def wx_send(q):
        cols = pl.ds(pl.multiple_of((1 - low) * HC, HC), HC)
        dst = wx.at[pl.ds(pl.multiple_of(q * WX_ROWS, WX_ROWS), WX_ROWS)]

        @pl.when(q * WX_ROWS < QW)
        def _():
            to_sib(wo.at[L - 1, pl.ds(pl.multiple_of(q * WX_ROWS, WX_ROWS), WX_ROWS), cols], dst, wx_sem).start()

        @pl.when(jnp.logical_and(q * WX_ROWS >= QW, q < WX_N))
        def _():
            to_sib(wd.at[L - 1, pl.ds(pl.multiple_of(q * WX_ROWS - QW, WX_ROWS), WX_ROWS), cols], dst, wx_sem).start()

    def wx_all():
        return to_sib(wx, wx, wx_sem)

    def hx_copy(start_col, n):
        cols = pl.ds(pl.multiple_of(start_col, 128), n)
        return to_sib(hid.at[:, cols], hsib.at[:, cols], hx_sem)

    def hx_all():
        return to_sib(hid, hsib, hx_sem)

    def xx_copy():
        cols = pl.ds(pl.multiple_of((1 - low) * HC, HC), HC)
        return to_sib(xres.at[CHUNKS - 1, :, cols], recv.at[CHUNKS - 1, 2, :, pl.ds(0, HC)], xx_sem)

    def half_share(q, j):
        return pltpu.make_async_remote_copy(
            src_ref=share.at[rows_of((1 - half) * 2 + q), half_cols(low, j)],
            dst_ref=recv.at[CHUNKS - 1, q, :, half_cols(0, j)],
            send_sem=rs_send.at[q], recv_sem=rs_recv.at[CHUNKS - 1, q, j],
            device_id={"tp": cross}, device_id_type=MESH)

    def gather_copy(c, k):
        block = rows_of(cross) if k == 2 else my_rows
        to = cross if k == 1 else sib
        return pltpu.make_async_remote_copy(
            src_ref=act.at[c, block], dst_ref=act.at[c, block],
            send_sem=ag_send.at[c, k], recv_sem=ag_recv.at[c, k],
            device_id={"tp": to}, device_id_type=MESH)

    def gain_row(l):
        rows = gain[...].astype(F32)
        row = rows[0:1]
        for i in range(1, L):
            row = jnp.where(l >= i, rows[i:i + 1], row)
        return row

    def normed(xf, grow):
        inv = lax.rsqrt(jnp.mean(xf * xf, axis=-1, keepdims=True) + NORM_EPS)
        return xf * inv * grow

    def groups_of(r, base):
        return [pl.ds(pl.multiple_of(base + (r * UNROLL + i) * ROWS, ROWS), ROWS) for i in range(UNROLL)]

    def sum_and_send(l, c):
        def arrived(j, carry):
            for k in range(3):
                share_copy(c, k, j).wait_recv()
            return carry

        lax.fori_loop(0, PIECES, arrived, 0)
        last = l == L - 1
        grow = gain_row(l + 1)

        def step(r, carry):
            rows, owns = groups_of(r, 0), groups_of(r, me * Q)
            new = []
            for rr, own in zip(rows, owns):
                s = share[own, :].astype(F32)
                for k in range(3):
                    s = s + recv[c, k, rr, :].astype(F32)
                xn = (xres[c, rr, :].astype(F32) + s).astype(BF16)
                xf = xn.astype(F32)
                new.append((xn, jnp.where(last, xf, normed(xf, grow)).astype(BF16)))
            for rr, own, (xn, a) in zip(rows, owns, new):
                xres[c, rr, :] = xn
                act[c, own, :] = a
            return carry

        lax.fori_loop(0, Q // (ROWS * UNROLL), step, 0)
        gather_copy(c, 1).start()
        gather_copy(c, 0).start()

    def forward(c):
        gather_copy(c, 1).wait_recv()
        gather_copy(c, 2).start()

    def gathered(c):
        gather_copy(c, 0).wait_recv()
        gather_copy(c, 2).wait_recv()
        for k in range(3):
            gather_copy(c, k).wait_send()

    def x_copy(c):
        return pltpu.make_async_copy(x_in.at[pl.ds(pl.multiple_of(c * M, M), M)], act.at[c], io_sem.at[c])

    res_copies = [pltpu.make_async_copy(x_in.at[pl.ds(pl.multiple_of(c * M + me * Q, Q), Q)], xres.at[c], io_sem.at[CHUNKS + c])
                  for c in range(CHUNKS)]
    x_copy(0).start()
    start(sp_copies(0))
    start(qk_copies(0))
    start(kv_copies(0, 0, 0, 0))
    for c in range(1, CHUNKS):
        x_copy(c).start()
    start(res_copies)

    barrier = pltpu.get_barrier_semaphore()
    for p in peers:
        pl.semaphore_signal(barrier, inc=1, device_id={"tp": p}, device_id_type=MESH)
    pl.semaphore_wait(barrier, 3)

    grow0 = gain_row(0)

    def first_norm(c):
        x_copy(c).wait()

        def step(r, carry):
            rows = groups_of(r, 0)
            new = [normed(act[c, rr, :].astype(F32), grow0).astype(BF16) for rr in rows]
            for rr, a in zip(rows, new):
                act[c, rr, :] = a
            return carry

        lax.fori_loop(0, M // (ROWS * UNROLL), step, 0)

    wait(res_copies)

    lane = lax.broadcasted_iota(jnp.int32, (GRP, 128), 1)
    trow = lax.broadcasted_iota(jnp.int32, (GRP, 128), 0)
    pos = lane % SEQ
    quad = 128 // SEQ
    in_group = (lane // SEQ) == (trow % quad)
    tgrp = trow // quad
    NG = GRP // quad
    scale = HD ** -0.5

    first_half = lane < HD // 2
    groups = range(KV_TOK // GRP)

    def toks(base, b, g):
        return pl.ds(pl.multiple_of(base + b * KV_TOK + g * GRP, GRP), GRP)

    def attend_scores(c, b, slot, g):
        rr, tr = toks(0, b, g), toks(c * M, b, g)
        cs = cs_t[tr, :]
        sc = pltpu.roll(cs, HD // 2, 1)
        co = jnp.where(first_half, cs, sc)
        si = jnp.where(first_half, -sc, cs)

        def rot(z):
            zf = z.astype(F32)
            return (zf * co + pltpu.roll(zf, HD // 2, 1) * si).astype(BF16)

        kr = rot(qk[rr, pl.ds(QW, HD)]).astype(F32)
        qs = jnp.concatenate([rot(qk[rr, pl.ds(h * HD, HD)]) for h in range(NH)], axis=0)
        kb = kbuf[slot, pl.ds(g * GRP, GRP)].reshape(GRP * SEQ, HD)
        s = lax.dot_general(qs, kb, (((1,), (1,)), ((), ())), preferred_element_type=F32)
        s = s.reshape(NH, GRP, GRP * SEQ)
        lg = s[:, :, 0:128]
        for n in range(1, NG):
            lg = jnp.where((tgrp == n)[None], s[:, :, n * 128:(n + 1) * 128], lg)
        ok = jnp.logical_and(in_group, pos < lens[tr, :])
        logit[g] = jnp.where(ok[None], lg * scale, -jnp.inf)
        selfl = jnp.sum(qs.reshape(NH, GRP, HD).astype(F32) * kr[None], axis=-1, keepdims=True) * scale
        selfp[g] = jnp.broadcast_to(selfl, (NH, GRP, HD))

    def attend_softmax(g):
        lg = logit[g]
        self_l = selfp[g]
        peak = jnp.maximum(jnp.max(lg, axis=-1, keepdims=True), self_l)
        w = jnp.exp(lg - peak)
        ws = jnp.exp(self_l - peak)
        den = jnp.sum(w, axis=-1, keepdims=True) + ws
        p = w / den
        selfp[g] = (ws / den).astype(BF16).astype(F32)
        pe = jnp.concatenate([jnp.where((tgrp == n)[None], p, 0.0) for n in range(NG)], axis=-1)
        prob[g] = pe.astype(BF16).reshape(NH * GRP, GRP * SEQ)

    def attend_values(b, slot, g):
        rr = toks(0, b, g)
        vb = vbuf[slot, pl.ds(g * GRP, GRP)].reshape(GRP * SEQ, HD)
        o = jnp.dot(prob[g], vb, preferred_element_type=F32).reshape(NH, GRP, HD)
        o = (o + selfp[g] * vnew[rr, :].astype(F32)[None]).astype(BF16)
        for h in range(NH):
            hid[rr, pl.ds(h * HD, HD)] = o[h]

    def glu(gate, up):
        gf = gate.astype(BF16).astype(F32)
        uf = up.astype(BF16).astype(F32)
        return (gf * jax.nn.sigmoid(gf) * uf).astype(BF16)

    def dot(a, b):
        return jnp.dot(a, b, preferred_element_type=F32)

    def body(it, carry):
        l = it // CHUNKS
        c = it % CHUNKS
        pc = (it + CHUNKS - 1) % CHUNKS
        plr = (it + CHUNKS - 1) // CHUNKS - 1
        nl = (it + 1) // CHUNKS
        nc = (it + 1) % CHUNKS

        @pl.when(it < CHUNKS)
        def _():
            first_norm(c)

        @pl.when(it >= CHUNKS)
        def _():
            gathered(c)

        @pl.when(it < iters - 1)
        def _():
            start(dn_copies(l, 0, 0))

        @pl.when(it == iters - 1)
        def _():
            wx_all().wait_recv()
            xx_copy().start()
            start(dn2_copies(0, 0))

        wait(sp_copies(l))
        r = dot(act[c], w1[1, :, pl.ds(0, HD + 2 * REM)])
        vnew[...] = r[:, :HD].astype(BF16)
        hid[:, pl.ds(QW + GU_N * GU_TILE, REM)] = glu(r[:, HD:HD + REM], r[:, HD + REM:])
        wait(qk_copies(l))
        start(gu_copies(l, 0, 1))
        for n in range((QW + HD) // SUB):
            qk[:, pl.ds(n * SUB, SUB)] = dot(act[c], w1[0, :, pl.ds(n * SUB, SUB)]).astype(BF16)

        @pl.when(it < iters - 1)
        def _():
            start(dn_copies(l, 1, 1))

        @pl.when(it == iters - 1)
        def _():
            start(dn2_copies(1, 1))
            hx_copy(QW + GU_N * GU_TILE, REM).start()


        def gu_step(j, carry, attend):
            slot = (j + 1) % 2
            kvs = j % 2

            if attend:
                @pl.when(j + 1 < KV_N)
                def _():
                    start(kv_copies(l, c, j + 1, 1 - kvs))

            @pl.when(j + 1 < GU_N)
            def _():
                start(gu_copies(l, j + 1, 1 - slot))

            @pl.when(jnp.logical_and(j + 1 == GU_N, it + 1 < iters))
            def _():
                start(qk_copies(nl))
                start(kv_copies(nl, nc, 0, 0))

            @pl.when(jnp.logical_and(j == HOOK_SUM, it > 0))
            def _():
                sum_and_send(plr, pc)

            @pl.when(it < iters - 1)
            def _():
                for i in range(WX_PER):
                    wx_send((it * GU_N + j) * WX_PER + i)

            @pl.when(jnp.logical_and(it == iters - 1, j > 0))
            def _():
                hx_copy(QW + (j - 1) * GU_TILE, GU_TILE).start()

            wait(gu_copies(l, j, slot))
            if attend:
                wait(kv_copies(l, c, j, kvs))
            stages = [lambda g: attend_scores(c, j, kvs, g), attend_softmax, lambda g: attend_values(j, kvs, g)]
            for n in range(GU_TILE // SUB):
                gu = []
                for half_cols in (0, GU_TILE):
                    gu.append(dot(act[c], w1[slot, :, pl.ds(half_cols + n * SUB, SUB)]))
                    if attend and stages:
                        stage = stages.pop(0)
                        for g in groups:
                            stage(g)
                hid[:, pl.ds(pl.multiple_of(QW + j * GU_TILE + n * SUB, 128), SUB)] = glu(*gu)
            return carry

        lax.fori_loop(0, KV_N, functools.partial(gu_step, attend=True), 0)

        @pl.when(it == iters - 1)
        def _():
            hx_copy(0, QW).start()

        lax.fori_loop(KV_N, GU_N, functools.partial(gu_step, attend=False), 0)

        @pl.when(it == iters - 1)
        def _():
            hx_copy(QW + (GU_N - 1) * GU_TILE, GU_TILE).start()


        @pl.when(it > 0)
        def _():
            for k in range(3):
                share_all(pc, k).wait_send()

        @pl.when(it + 1 < iters)
        def _():
            start(sp_copies(nl))

        def dn_step(j, carry):
            slot = j % 2

            @pl.when(jnp.logical_and(j == HOOK_FWD, it > 0))
            def _():
                forward(pc)

            wait(dn_copies(l, j, slot))
            for n in range(PER):
                share[:, pl.ds(pl.multiple_of(j * DN_TILE + n * SUB, SUB), SUB)] = dot(
                    hid[...], w2[slot, :, pl.ds(n * SUB, SUB)]).astype(BF16)

            @pl.when(j + 2 < DN_N)
            def _():
                start(dn_copies(l, j + 2, slot))

            @pl.when(j > 0)
            def _():
                send_piece(c, j * PER - 1)

            for n in range(PER - 1):
                send_piece(c, j * PER + n)
            return carry

        def dn2_step(j, carry):
            slot = j % 2

            @pl.when(j == HOOK_FWD)
            def _():
                forward(pc)

            wait(dn2_copies(j, slot))
            for m in range(0, M, SUB):
                rows = pl.ds(m, SUB)
                t = dot(hid[rows, :], w2[slot, :, pl.ds(0, SUB)])
                if m == 0:
                    @pl.when(j == 0)
                    def _():
                        hx_all().wait_recv()
                share[rows, half_cols(low, j)] = (t + dot(hsib[rows, :], w2[slot, :, pl.ds(SUB, SUB)])).astype(BF16)

            @pl.when(j + 2 < HP)
            def _():
                start(dn2_copies(j + 2, slot))

            @pl.when(j > 0)
            def _():
                for q in range(2):
                    half_share(q, j - 1).start()
            return carry

        @pl.when(it < iters - 1)
        def _():
            lax.fori_loop(0, DN_N, dn_step, 0)
            send_piece(c, PIECES - 1)

        @pl.when(it == iters - 1)
        def _():
            lax.fori_loop(0, HP, dn2_step, 0)
            for q in range(2):
                half_share(q, HP - 1).start()
        return carry

    lax.fori_loop(0, iters, body, 0)

    fc = (iters - 1) % CHUNKS

    def final_copy(k, j):
        rows = pl.ds(pl.multiple_of(((1 - half) if k == 2 else half) * HR, HR), HR)
        ref = act.at[fc, rows, half_cols(low, j)]
        return pltpu.make_async_remote_copy(
            src_ref=ref, dst_ref=ref, send_sem=fin_send.at[k], recv_sem=fin_recv.at[k, j],
            device_id={"tp": cross if k == 1 else sib}, device_id_type=MESH)

    def out_copy(j, core):
        cols = half_cols(core, j)
        return pltpu.make_async_copy(act.at[fc, :, cols], out.at[pl.ds(fc * M, M), cols], io_sem.at[fc])

    out_copies = []
    for c in range(CHUNKS):
        if c != fc:
            gathered(c)
            cp = pltpu.make_async_copy(act.at[c], out.at[pl.ds(c * M, M)], io_sem.at[c])
            cp.start()
            out_copies.append(cp)
    xx_copy().wait()

    def final_sum(j, carry):
        cols, got = half_cols(low, j), half_cols(0, j)
        for q in range(2):
            half_share(q, j).wait_recv()
            mine = low == q
            for r in range(0, Q, ROWS):
                rows = pl.ds(pl.multiple_of((half * 2 + q) * Q + r, ROWS), ROWS)
                rr = pl.ds(r, ROWS)
                t = share[rows, cols].astype(F32) + recv[fc, q, rr, got].astype(F32)
                x = jnp.where(mine, xres[fc, rr, cols].astype(F32), recv[fc, 2, rr, got].astype(F32))
                act[fc, rows, cols] = (x + t).astype(BF16)
        final_copy(1, j).start()
        final_copy(0, j).start()
        return carry

    lax.fori_loop(0, HP, final_sum, 0)

    def final_forward(j, carry):
        @pl.when(j < HP)
        def _():
            final_copy(1, j).wait_recv()
            final_copy(2, j).start()
            out_copy(j, low).start()

        @pl.when(j > 0)
        def _():
            final_copy(0, j - 1).wait_recv()
            final_copy(2, j - 1).wait_recv()
            out_copy(j - 1, 1 - low).start()
        return carry

    lax.fori_loop(0, HP + 1, final_forward, 0)

    own_cols = pl.ds(pl.multiple_of(low * HC, HC), HC)
    for q in range(2):
        pltpu.make_async_remote_copy(
            src_ref=share.at[rows_of((1 - half) * 2 + q), own_cols], dst_ref=recv.at[fc, q, :, pl.ds(0, HC)],
            send_sem=rs_send.at[q], recv_sem=rs_recv.at[fc, q, 0],
            device_id={"tp": cross}, device_id_type=MESH).wait_send()
    for k in range(3):
        rows = pl.ds(pl.multiple_of(((1 - half) if k == 2 else half) * HR, HR), HR)
        ref = act.at[fc, rows, own_cols]
        pltpu.make_async_remote_copy(
            src_ref=ref, dst_ref=ref, send_sem=fin_send.at[k], recv_sem=fin_recv.at[k, 0],
            device_id={"tp": cross if k == 1 else sib}, device_id_type=MESH).wait_send()
    wx_all().wait_send()
    hx_all().wait_send()
    pltpu.make_async_copy(act.at[fc], out.at[pl.ds(fc * M, M)], io_sem.at[fc]).wait()
    wait(out_copies)


def solution(mesh):
    tp_size = mesh.shape['tp']
    arg_specs = (P('dp', None), P('dp'), P(), P(None, None, 'tp'), P(None, None, 'tp'), P(None, None, 'tp'), P(None, 'tp', None), P(None, None, 'tp'), P(None, None, 'tp'), P(None, 'tp', None), P(None, 'dp', None, 'tp', None), P(None, 'dp', None, 'tp', None))

    def per_device(x_in, lengths, norm_gain, w_q, w_k, w_v, w_o, w_gate, w_up, w_down, k_cache, v_cache):
        L, tok, seq, kvh, hd = k_cache.shape
        D = x_in.shape[1]
        qw = w_q.shape[2]
        ff = w_gate.shape[2]
        inv_freq = 1.0 / (ROPE_BASE ** (jnp.arange(0, hd, 2).astype(F32) / hd))
        ang = lengths.astype(F32)[:, None] * inv_freq[None, :]
        cs_t = jnp.concatenate([jnp.cos(ang), jnp.sin(ang)], axis=-1)
        lens = jnp.broadcast_to(lengths[:, None], (tok, 128))
        kc = k_cache.reshape(L, tok, seq, hd)
        vc = v_cache.reshape(L, tok, seq, hd)
        M = tok // CHUNKS
        Q = M // tp_size
        vmem = pl.BlockSpec(memory_space=pltpu.VMEM)
        hbm = pl.BlockSpec(memory_space=pl.ANY)
        dma = pltpu.SemaphoreType.DMA
        return pl.pallas_call(
            functools.partial(layers_kernel, tp_size, (L, tok, D, qw, hd, ff, seq)),
            out_shape=[jax.ShapeDtypeStruct((tok, D), BF16), jax.ShapeDtypeStruct((qw + ff, D // 2), BF16)],
            in_specs=[hbm, vmem, vmem, vmem] + [hbm] * 9,
            out_specs=[hbm, hbm],
            scratch_shapes=[
                pltpu.VMEM((CHUNKS, M, D), BF16),
                pltpu.VMEM((2, D, 2 * GU_TILE), BF16),
                pltpu.VMEM((2, qw + ff, DN_TILE), BF16),
                pltpu.VMEM((M, qw + ff), BF16),
                pltpu.VMEM((M, qw + hd), BF16),
                pltpu.VMEM((M, hd), BF16),
                pltpu.VMEM((2, KV_TOK, seq, hd), BF16),
                pltpu.VMEM((2, KV_TOK, seq, hd), BF16),
                pltpu.VMEM((M, D), BF16),
                pltpu.VMEM((CHUNKS, 3, Q, D), BF16),
                pltpu.VMEM((CHUNKS, Q, D), BF16),
                pltpu.VMEM((KV_TOK // GRP, qw // hd, GRP, hd), F32),
                pltpu.VMEM((KV_TOK // GRP, qw // hd, GRP, hd), F32),
                pltpu.VMEM((KV_TOK // GRP, qw // hd * GRP, GRP * seq), BF16),
                pltpu.VMEM((M, qw + ff), BF16),
                dma((2, 2)), dma((3,)), dma((2, 3)), dma((2, 2)), dma((2 * CHUNKS,)),
                dma((3,)), dma((CHUNKS, 3, D // SUB)), dma((CHUNKS, 3)), dma((CHUNKS, 3)),
                dma((3,)), dma((3, D // SUB)), dma((2,)), dma((2,)), dma((2,)),
            ],
            compiler_params=pltpu.CompilerParams(
                collective_id=0, has_side_effects=True, vmem_limit_bytes=67043328),
            name="layers",
        )(x_in, lens, cs_t, norm_gain, w_q, w_k, w_v, w_o, w_gate, w_up, w_down, kc, vc)[0]

    return jax.shard_map(per_device, mesh=mesh, in_specs=arg_specs, out_specs=P('dp', None), check_vma=False)
```

```python
import functools

import jax
import jax.numpy as jnp
from jax import lax
from jax.experimental import pallas as pl
from jax.experimental.pallas import tpu as pltpu
from jax.sharding import PartitionSpec as P

NORM_EPS = 1e-5
ROPE_BASE = 500000.0
MESH = pl.DeviceIdType.MESH
F32 = jnp.float32
BF16 = jnp.bfloat16

CHUNKS = 2
GU_TILE = 512
DN_TILE = 512
SUB = 256
KV_TOK = 64
GRP = 16
ROWS = 16
UNROLL = 2
LAG = 3
HOOK_SUM = 5
HOOK_FWD = 3


def layers_kernel(tp, dims, *refs):
    (x_in, len_in, freq, gain, wq, wk, wv, wo, wg, wu, wd, kc, vc, out, wx,
     act, w1, w2, hid, qk, vnew, kbuf, vbuf, share, recv, xres, logit, selfp, prob, hsib, lens, cs_t,
     w1_sem, wsp_sem, w2_sem, kv_sem, io_sem, rs_send, rs_recv, ag_send, ag_recv, fin_send, fin_recv,
     wx_sem, hx_sem, xx_sem) = refs
    L, tok, D, QW, HD, FF, SEQ = dims
    M = tok // CHUNKS
    Q = M // tp
    NH = QW // HD
    iters = L * CHUNKS
    GU_N = FF // GU_TILE
    REM = FF - GU_N * GU_TILE
    DN_N = D // DN_TILE
    PIECES = D // SUB
    PER = DN_TILE // SUB
    HC = D // 2
    HR = M // 2
    HP = HC // SUB
    WX_ROWS = 128
    WX_N = (QW + FF) // WX_ROWS
    WX_PER = -(-WX_N // ((iters - 1) * (GU_N + DN_N)))
    KV_N = M // KV_TOK

    me = lax.axis_index("tp")
    half = me // 2
    low = me - half * 2
    sib = half * 2 + (1 - low)
    cross = (1 - half) * 2 + low
    diag = (1 - half) * 2 + (1 - low)
    peers = (sib, cross, diag)
    my_rows = pl.ds(pl.multiple_of(me * Q, Q), Q)

    def rows_of(dev):
        return pl.ds(pl.multiple_of(dev * Q, Q), Q)

    def qk_copies(l):
        return [pltpu.make_async_copy(wq.at[l], w1.at[0, :, pl.ds(0, QW)], w1_sem.at[0, 0]),
                pltpu.make_async_copy(wk.at[l], w1.at[0, :, pl.ds(QW, HD)], w1_sem.at[0, 1])]

    def gu_copies(l, j, slot):
        cols = pl.ds(pl.multiple_of(j * GU_TILE, GU_TILE), GU_TILE)
        return [pltpu.make_async_copy(wg.at[l, :, cols], w1.at[slot, :, pl.ds(0, GU_TILE)], w1_sem.at[slot, 0]),
                pltpu.make_async_copy(wu.at[l, :, cols], w1.at[slot, :, pl.ds(GU_TILE, GU_TILE)], w1_sem.at[slot, 1])]

    def sp_copies(l):
        rem = pl.ds(GU_N * GU_TILE, REM)
        return [pltpu.make_async_copy(wv.at[l], w1.at[1, :, pl.ds(0, HD)], wsp_sem.at[0]),
                pltpu.make_async_copy(wg.at[l, :, rem], w1.at[1, :, pl.ds(HD, REM)], wsp_sem.at[1]),
                pltpu.make_async_copy(wu.at[l, :, rem], w1.at[1, :, pl.ds(HD + REM, REM)], wsp_sem.at[2])]

    def dn_copies(l, j, slot):
        cols = pl.ds(pl.multiple_of(j * DN_TILE, DN_TILE), DN_TILE)
        return [pltpu.make_async_copy(wo.at[l, :, cols], w2.at[slot, pl.ds(0, QW)], w2_sem.at[slot, 0]),
                pltpu.make_async_copy(wd.at[l, :, cols], w2.at[slot, pl.ds(QW, FF)], w2_sem.at[slot, 1])]

    def half_cols(core, j):
        return pl.ds(pl.multiple_of(core * HC + j * SUB, SUB), SUB)

    def dn2_copies(j, slot):
        own, got = half_cols(low, j), pl.ds(pl.multiple_of(j * SUB, SUB), SUB)
        return [pltpu.make_async_copy(wo.at[L - 1, :, own], w2.at[slot, pl.ds(0, QW), pl.ds(0, SUB)], w2_sem.at[slot, 0]),
                pltpu.make_async_copy(wd.at[L - 1, :, own], w2.at[slot, pl.ds(QW, FF), pl.ds(0, SUB)], w2_sem.at[slot, 1]),
                pltpu.make_async_copy(wx.at[:, got], w2.at[slot, :, pl.ds(SUB, SUB)], w2_sem.at[slot, 2])]

    def kv_copies(l, c, b, slot):
        toks = pl.ds(pl.multiple_of(c * M + b * KV_TOK, KV_TOK), KV_TOK)
        return [pltpu.make_async_copy(kc.at[l, toks], kbuf.at[slot], kv_sem.at[slot, 0]),
                pltpu.make_async_copy(vc.at[l, toks], vbuf.at[slot], kv_sem.at[slot, 1])]

    def start(copies):
        for cp in copies:
            cp.start()

    def wait(copies):
        for cp in copies:
            cp.wait()

    def piece(p):
        return pl.ds(pl.multiple_of(p * SUB, SUB), SUB)

    def share_copy(c, k, j):
        cols = piece(j)
        return pltpu.make_async_remote_copy(
            src_ref=share.at[rows_of(peers[k]), cols], dst_ref=recv.at[c, k, :, cols],
            send_sem=rs_send.at[k], recv_sem=rs_recv.at[c, k, j],
            device_id={"tp": peers[k]}, device_id_type=MESH)

    def send_piece(c, j):
        for k in (1, 2, 0):
            share_copy(c, k, j).start()

    def share_all(c, k):
        return pltpu.make_async_remote_copy(
            src_ref=share.at[rows_of(peers[k])], dst_ref=recv.at[c, k],
            send_sem=rs_send.at[k], recv_sem=rs_recv.at[c, k, 0],
            device_id={"tp": peers[k]}, device_id_type=MESH)

    def to_sib(src, dst, sems):
        return pltpu.make_async_remote_copy(
            src_ref=src, dst_ref=dst, send_sem=sems.at[0], recv_sem=sems.at[1],
            device_id={"tp": sib}, device_id_type=MESH)

    def wx_send(q):
        cols = pl.ds(pl.multiple_of((1 - low) * HC, HC), HC)
        dst = wx.at[pl.ds(pl.multiple_of(q * WX_ROWS, WX_ROWS), WX_ROWS)]

        @pl.when(q * WX_ROWS < QW)
        def _():
            to_sib(wo.at[L - 1, pl.ds(pl.multiple_of(q * WX_ROWS, WX_ROWS), WX_ROWS), cols], dst, wx_sem).start()

        @pl.when(jnp.logical_and(q * WX_ROWS >= QW, q < WX_N))
        def _():
            to_sib(wd.at[L - 1, pl.ds(pl.multiple_of(q * WX_ROWS - QW, WX_ROWS), WX_ROWS), cols], dst, wx_sem).start()

    def wx_all():
        return to_sib(wx, wx, wx_sem)

    def hx_copy(start_col, n):
        cols = pl.ds(pl.multiple_of(start_col, 128), n)
        return to_sib(hid.at[:, cols], hsib.at[:, cols], hx_sem)

    def hx_all():
        return to_sib(hid, hsib, hx_sem)

    def xx_copy():
        cols = pl.ds(pl.multiple_of((1 - low) * HC, HC), HC)
        return to_sib(xres.at[CHUNKS - 1, :, cols], recv.at[CHUNKS - 1, 2, :, pl.ds(0, HC)], xx_sem)

    def half_share(q, j):
        return pltpu.make_async_remote_copy(
            src_ref=share.at[rows_of((1 - half) * 2 + q), half_cols(low, j)],
            dst_ref=recv.at[CHUNKS - 1, q, :, half_cols(0, j)],
            send_sem=rs_send.at[q], recv_sem=rs_recv.at[CHUNKS - 1, q, j],
            device_id={"tp": cross}, device_id_type=MESH)

    def gather_copy(c, k):
        block = rows_of(cross) if k == 2 else my_rows
        to = cross if k == 1 else sib
        return pltpu.make_async_remote_copy(
            src_ref=act.at[c, block], dst_ref=act.at[c, block],
            send_sem=ag_send.at[c, k], recv_sem=ag_recv.at[c, k],
            device_id={"tp": to}, device_id_type=MESH)

    def gain_row(l):
        rows = gain[...].astype(F32)
        row = rows[0:1]
        for i in range(1, L):
            row = jnp.where(l >= i, rows[i:i + 1], row)
        return row

    def normed(xf, grow):
        inv = lax.rsqrt(jnp.mean(xf * xf, axis=-1, keepdims=True) + NORM_EPS)
        return xf * inv * grow

    def groups_of(r, base):
        return [pl.ds(pl.multiple_of(base + (r * UNROLL + i) * ROWS, ROWS), ROWS) for i in range(UNROLL)]

    def sum_and_send(l, c):
        def arrived(j, carry):
            for k in range(3):
                share_copy(c, k, j).wait_recv()
            return carry

        lax.fori_loop(0, PIECES, arrived, 0)
        last = l == L - 1
        grow = gain_row(l + 1)

        def step(r, carry):
            rows, owns = groups_of(r, 0), groups_of(r, me * Q)
            new = []
            for rr, own in zip(rows, owns):
                s = share[own, :].astype(F32)
                for k in range(3):
                    s = s + recv[c, k, rr, :].astype(F32)
                xn = (xres[c, rr, :].astype(F32) + s).astype(BF16)
                xf = xn.astype(F32)
                new.append((xn, jnp.where(last, xf, normed(xf, grow)).astype(BF16)))
            for rr, own, (xn, a) in zip(rows, owns, new):
                xres[c, rr, :] = xn
                act[c, own, :] = a
            return carry

        lax.fori_loop(0, Q // (ROWS * UNROLL), step, 0)
        gather_copy(c, 1).start()
        gather_copy(c, 0).start()

    def forward(c):
        gather_copy(c, 1).wait_recv()
        gather_copy(c, 2).start()

    def gathered(c):
        gather_copy(c, 0).wait_recv()
        gather_copy(c, 2).wait_recv()
        for k in range(3):
            gather_copy(c, k).wait_send()

    def x_copy(c):
        return pltpu.make_async_copy(x_in.at[pl.ds(pl.multiple_of(c * M, M), M)], act.at[c], io_sem.at[c])

    res_copies = [pltpu.make_async_copy(x_in.at[pl.ds(pl.multiple_of(c * M + me * Q, Q), Q)], xres.at[c], io_sem.at[CHUNKS + c])
                  for c in range(CHUNKS)]
    x_copy(0).start()
    start(sp_copies(0))
    start(qk_copies(0))
    start(kv_copies(0, 0, 0, 0))
    for c in range(1, CHUNKS):
        x_copy(c).start()
    start(res_copies)

    barrier = pltpu.get_barrier_semaphore()
    for p in peers:
        pl.semaphore_signal(barrier, inc=1, device_id={"tp": p}, device_id_type=MESH)
    pl.semaphore_wait(barrier, 3)

    grow0 = gain_row(0)

    def first_norm(c):
        x_copy(c).wait()

        def step(r, carry):
            rows = groups_of(r, 0)
            new = [normed(act[c, rr, :].astype(F32), grow0).astype(BF16) for rr in rows]
            for rr, a in zip(rows, new):
                act[c, rr, :] = a
            return carry

        lax.fori_loop(0, M // (ROWS * UNROLL), step, 0)


    def table(i, carry):
        rows = pl.ds(pl.multiple_of(i * 128, 128), 128)
        row = len_in[pl.ds(i, 1), :].astype(F32)
        by_token = jnp.broadcast_to(row, (128, 128)).T
        ang = by_token * freq[...]
        lens[rows, :] = by_token.astype(jnp.int32)
        lanes = lax.broadcasted_iota(jnp.int32, (128, 128), 1)
        cs_t[rows, :] = jnp.where(lanes < HD // 2, jnp.cos(ang), jnp.sin(ang))
        return carry

    lax.fori_loop(0, tok // 128, table, 0)

    lane = lax.broadcasted_iota(jnp.int32, (GRP, 128), 1)
    trow = lax.broadcasted_iota(jnp.int32, (GRP, 128), 0)
    pos = lane % SEQ
    quad = 128 // SEQ
    in_group = (lane // SEQ) == (trow % quad)
    tgrp = trow // quad
    NG = GRP // quad
    scale = HD ** -0.5

    first_half = lane < HD // 2
    groups = range(KV_TOK // GRP)

    def toks(base, b, g):
        return pl.ds(pl.multiple_of(base + b * KV_TOK + g * GRP, GRP), GRP)

    def attend_scores(c, b, slot, g):
        rr, tr = toks(0, b, g), toks(c * M, b, g)
        cs = cs_t[tr, :]
        sc = pltpu.roll(cs, HD // 2, 1)
        co = jnp.where(first_half, cs, sc)
        si = jnp.where(first_half, -sc, cs)

        def rot(z):
            zf = z.astype(F32)
            return (zf * co + pltpu.roll(zf, HD // 2, 1) * si).astype(BF16)

        kr = rot(qk[rr, pl.ds(QW, HD)]).astype(F32)
        qs = jnp.concatenate([rot(qk[rr, pl.ds(h * HD, HD)]) for h in range(NH)], axis=0)
        kb = kbuf[slot, pl.ds(g * GRP, GRP)].reshape(GRP * SEQ, HD)
        s = lax.dot_general(qs, kb, (((1,), (1,)), ((), ())), preferred_element_type=F32)
        s = s.reshape(NH, GRP, GRP * SEQ)
        lg = s[:, :, 0:128]
        for n in range(1, NG):
            lg = jnp.where((tgrp == n)[None], s[:, :, n * 128:(n + 1) * 128], lg)
        ok = jnp.logical_and(in_group, pos < lens[tr, :])
        logit[g] = jnp.where(ok[None], lg * scale, -jnp.inf)
        selfl = jnp.sum(qs.reshape(NH, GRP, HD).astype(F32) * kr[None], axis=-1, keepdims=True) * scale
        selfp[g] = jnp.broadcast_to(selfl, (NH, GRP, HD))

    def attend_softmax(g):
        lg = logit[g]
        self_l = selfp[g]
        peak = jnp.maximum(jnp.max(lg, axis=-1, keepdims=True), self_l)
        w = jnp.exp(lg - peak)
        ws = jnp.exp(self_l - peak)
        den = jnp.sum(w, axis=-1, keepdims=True) + ws
        p = w / den
        selfp[g] = (ws / den).astype(BF16).astype(F32)
        pe = jnp.concatenate([jnp.where((tgrp == n)[None], p, 0.0) for n in range(NG)], axis=-1)
        prob[g] = pe.astype(BF16).reshape(NH * GRP, GRP * SEQ)

    def attend_values(b, slot, g):
        rr = toks(0, b, g)
        vb = vbuf[slot, pl.ds(g * GRP, GRP)].reshape(GRP * SEQ, HD)
        o = jnp.dot(prob[g], vb, preferred_element_type=F32).reshape(NH, GRP, HD)
        o = (o + selfp[g] * vnew[rr, :].astype(F32)[None]).astype(BF16)
        for h in range(NH):
            hid[rr, pl.ds(h * HD, HD)] = o[h]

    def glu(gate, up):
        gf = gate.astype(BF16).astype(F32)
        uf = up.astype(BF16).astype(F32)
        return (gf * jax.nn.sigmoid(gf) * uf).astype(BF16)

    def dot(a, b):
        return jnp.dot(a, b, preferred_element_type=F32)

    fc = (iters - 1) % CHUNKS

    def final_copy(k, j):
        rows = pl.ds(pl.multiple_of(((1 - half) if k == 2 else half) * HR, HR), HR)
        ref = act.at[fc, rows, half_cols(low, j)]
        return pltpu.make_async_remote_copy(
            src_ref=ref, dst_ref=ref, send_sem=fin_send.at[k], recv_sem=fin_recv.at[k, j],
            device_id={"tp": cross if k == 1 else sib}, device_id_type=MESH)

    def final_sum(j, carry):
        cols, got = half_cols(low, j), half_cols(0, j)
        for q in range(2):
            half_share(q, j).wait_recv()
            mine = low == q
            for r in range(0, Q, ROWS):
                rows = pl.ds(pl.multiple_of((half * 2 + q) * Q + r, ROWS), ROWS)
                rr = pl.ds(r, ROWS)
                t = share[rows, cols].astype(F32) + recv[fc, q, rr, got].astype(F32)
                x = jnp.where(mine, xres[fc, rr, cols].astype(F32), recv[fc, 2, rr, got].astype(F32))
                act[fc, rows, cols] = (x + t).astype(BF16)
        final_copy(1, j).start()
        final_copy(0, j).start()
        return carry

    def body(it, carry):
        l = it // CHUNKS
        c = it % CHUNKS
        pc = (it + CHUNKS - 1) % CHUNKS
        plr = (it + CHUNKS - 1) // CHUNKS - 1
        nl = (it + 1) // CHUNKS
        nc = (it + 1) % CHUNKS

        @pl.when(it < CHUNKS)
        def _():
            first_norm(c)

        @pl.when(it == 1)
        def _():
            wait(res_copies)

        @pl.when(it >= CHUNKS)
        def _():
            gathered(c)

        @pl.when(it < iters - 1)
        def _():
            start(dn_copies(l, 0, 0))

        @pl.when(it == iters - 1)
        def _():
            wx_all().wait_recv()
            xx_copy().start()
            start(dn2_copies(0, 0))

        wait(sp_copies(l))
        r = dot(act[c], w1[1, :, pl.ds(0, HD + 2 * REM)])
        vnew[...] = r[:, :HD].astype(BF16)
        hid[:, pl.ds(QW + GU_N * GU_TILE, REM)] = glu(r[:, HD:HD + REM], r[:, HD + REM:])
        wait(qk_copies(l))
        start(gu_copies(l, 0, 1))
        for n in range((QW + HD) // SUB):
            qk[:, pl.ds(n * SUB, SUB)] = dot(act[c], w1[0, :, pl.ds(n * SUB, SUB)]).astype(BF16)

        @pl.when(it < iters - 1)
        def _():
            start(dn_copies(l, 1, 1))

        @pl.when(it == iters - 1)
        def _():
            start(dn2_copies(1, 1))
            hx_copy(QW + GU_N * GU_TILE, REM).start()


        def gu_step(j, carry, attend):
            slot = (j + 1) % 2
            kvs = j % 2

            if attend:
                @pl.when(j + 1 < KV_N)
                def _():
                    start(kv_copies(l, c, j + 1, 1 - kvs))

            @pl.when(j + 1 < GU_N)
            def _():
                start(gu_copies(l, j + 1, 1 - slot))

            @pl.when(jnp.logical_and(j + 1 == GU_N, it + 1 < iters))
            def _():
                start(qk_copies(nl))
                start(kv_copies(nl, nc, 0, 0))

            @pl.when(jnp.logical_and(j == HOOK_SUM, it > 0))
            def _():
                sum_and_send(plr, pc)

            @pl.when(it < iters - 1)
            def _():
                for i in range(WX_PER):
                    wx_send((it * (GU_N + DN_N) + j) * WX_PER + i)

            @pl.when(jnp.logical_and(it == iters - 1, j > 0))
            def _():
                hx_copy(QW + (j - 1) * GU_TILE, GU_TILE).start()

            wait(gu_copies(l, j, slot))
            if attend:
                wait(kv_copies(l, c, j, kvs))
            stages = [lambda g: attend_scores(c, j, kvs, g), attend_softmax, lambda g: attend_values(j, kvs, g)]
            for n in range(GU_TILE // SUB):
                gu = []
                for half_cols in (0, GU_TILE):
                    gu.append(dot(act[c], w1[slot, :, pl.ds(half_cols + n * SUB, SUB)]))
                    if attend and stages:
                        stage = stages.pop(0)
                        for g in groups:
                            stage(g)
                hid[:, pl.ds(pl.multiple_of(QW + j * GU_TILE + n * SUB, 128), SUB)] = glu(*gu)
            return carry

        lax.fori_loop(0, KV_N, functools.partial(gu_step, attend=True), 0)

        @pl.when(it == iters - 1)
        def _():
            hx_copy(0, QW).start()

        lax.fori_loop(KV_N, GU_N, functools.partial(gu_step, attend=False), 0)

        @pl.when(it == iters - 1)
        def _():
            hx_copy(QW + (GU_N - 1) * GU_TILE, GU_TILE).start()


        @pl.when(it > 0)
        def _():
            for k in range(3):
                share_all(pc, k).wait_send()

        @pl.when(it + 1 < iters)
        def _():
            start(sp_copies(nl))

        def dn_step(j, carry):
            slot = j % 2

            @pl.when(jnp.logical_and(j == HOOK_FWD, it > 0))
            def _():
                forward(pc)

            for i in range(WX_PER):
                wx_send((it * (GU_N + DN_N) + GU_N + j) * WX_PER + i)

            wait(dn_copies(l, j, slot))
            for n in range(PER):
                share[:, pl.ds(pl.multiple_of(j * DN_TILE + n * SUB, SUB), SUB)] = dot(
                    hid[...], w2[slot, :, pl.ds(n * SUB, SUB)]).astype(BF16)

            @pl.when(j + 2 < DN_N)
            def _():
                start(dn_copies(l, j + 2, slot))

            @pl.when(j > 0)
            def _():
                send_piece(c, j * PER - 1)

            for n in range(PER - 1):
                send_piece(c, j * PER + n)
            return carry

        def dn2_step(j, carry):
            slot = j % 2

            @pl.when(j == HOOK_FWD)
            def _():
                forward(pc)

            wait(dn2_copies(j, slot))
            for m in range(2):
                rows = pl.ds(pl.multiple_of((1 - half if m == 0 else half) * HR, HR), HR)
                t = dot(hid[rows, :], w2[slot, :, pl.ds(0, SUB)])
                if m == 0:
                    @pl.when(j == 0)
                    def _():
                        hx_all().wait_recv()
                share[rows, half_cols(low, j)] = (t + dot(hsib[rows, :], w2[slot, :, pl.ds(SUB, SUB)])).astype(BF16)

            @pl.when(j + 2 < HP)
            def _():
                start(dn2_copies(j + 2, slot))

            for q in range(2):
                half_share(q, j).start()

            @pl.when(j == LAG)
            def _():
                xx_copy().wait()

            @pl.when(j >= LAG)
            def _():
                final_sum(j - LAG, 0)
            return carry

        @pl.when(it < iters - 1)
        def _():
            lax.fori_loop(0, DN_N, dn_step, 0)
            send_piece(c, PIECES - 1)

        @pl.when(it == iters - 1)
        def _():
            lax.fori_loop(0, HP, dn2_step, 0)
        return carry

    lax.fori_loop(0, iters, body, 0)

    def out_copy(j, core):
        cols = half_cols(core, j)
        return pltpu.make_async_copy(act.at[fc, :, cols], out.at[pl.ds(fc * M, M), cols], io_sem.at[fc])

    out_copies = []
    for c in range(CHUNKS):
        if c != fc:
            gathered(c)
            cp = pltpu.make_async_copy(act.at[c], out.at[pl.ds(c * M, M)], io_sem.at[c])
            cp.start()
            out_copies.append(cp)

    lax.fori_loop(HP - LAG, HP, final_sum, 0)

    def final_forward(j, carry):
        @pl.when(j < HP)
        def _():
            final_copy(1, j).wait_recv()
            final_copy(2, j).start()
            out_copy(j, low).start()

        @pl.when(j > 0)
        def _():
            final_copy(0, j - 1).wait_recv()
            final_copy(2, j - 1).wait_recv()
            out_copy(j - 1, 1 - low).start()
        return carry

    lax.fori_loop(0, HP + 1, final_forward, 0)

    own_cols = pl.ds(pl.multiple_of(low * HC, HC), HC)
    for q in range(2):
        pltpu.make_async_remote_copy(
            src_ref=share.at[rows_of((1 - half) * 2 + q), own_cols], dst_ref=recv.at[fc, q, :, pl.ds(0, HC)],
            send_sem=rs_send.at[q], recv_sem=rs_recv.at[fc, q, 0],
            device_id={"tp": cross}, device_id_type=MESH).wait_send()
    for k in range(3):
        rows = pl.ds(pl.multiple_of(((1 - half) if k == 2 else half) * HR, HR), HR)
        ref = act.at[fc, rows, own_cols]
        pltpu.make_async_remote_copy(
            src_ref=ref, dst_ref=ref, send_sem=fin_send.at[k], recv_sem=fin_recv.at[k, 0],
            device_id={"tp": cross if k == 1 else sib}, device_id_type=MESH).wait_send()
    wx_all().wait_send()
    hx_all().wait_send()
    pltpu.make_async_copy(act.at[fc], out.at[pl.ds(fc * M, M)], io_sem.at[fc]).wait()
    wait(out_copies)


def solution(mesh):
    tp_size = mesh.shape['tp']
    arg_specs = (P('dp', None), P('dp'), P(), P(None, None, 'tp'), P(None, None, 'tp'), P(None, None, 'tp'), P(None, 'tp', None), P(None, None, 'tp'), P(None, None, 'tp'), P(None, 'tp', None), P(None, 'dp', None, 'tp', None), P(None, 'dp', None, 'tp', None))

    def per_device(x_in, lengths, norm_gain, w_q, w_k, w_v, w_o, w_gate, w_up, w_down, k_cache, v_cache):
        L, tok, seq, kvh, hd = k_cache.shape
        D = x_in.shape[1]
        qw = w_q.shape[2]
        ff = w_gate.shape[2]
        inv_freq = 1.0 / (ROPE_BASE ** (jnp.arange(0, hd, 2).astype(F32) / hd))
        freq = jnp.concatenate([inv_freq, inv_freq])[None, :]
        len_in = lengths.reshape(tok // 128, 128)
        kc = k_cache.reshape(L, tok, seq, hd)
        vc = v_cache.reshape(L, tok, seq, hd)
        M = tok // CHUNKS
        Q = M // tp_size
        vmem = pl.BlockSpec(memory_space=pltpu.VMEM)
        hbm = pl.BlockSpec(memory_space=pl.ANY)
        dma = pltpu.SemaphoreType.DMA
        return pl.pallas_call(
            functools.partial(layers_kernel, tp_size, (L, tok, D, qw, hd, ff, seq)),
            out_shape=[jax.ShapeDtypeStruct((tok, D), BF16), jax.ShapeDtypeStruct((qw + ff, D // 2), BF16)],
            in_specs=[hbm, vmem, vmem, vmem] + [hbm] * 9,
            out_specs=[hbm, hbm],
            scratch_shapes=[
                pltpu.VMEM((CHUNKS, M, D), BF16),
                pltpu.VMEM((2, D, 2 * GU_TILE), BF16),
                pltpu.VMEM((2, qw + ff, DN_TILE), BF16),
                pltpu.VMEM((M, qw + ff), BF16),
                pltpu.VMEM((M, qw + hd), BF16),
                pltpu.VMEM((M, hd), BF16),
                pltpu.VMEM((2, KV_TOK, seq, hd), BF16),
                pltpu.VMEM((2, KV_TOK, seq, hd), BF16),
                pltpu.VMEM((M, D), BF16),
                pltpu.VMEM((CHUNKS, 3, Q, D), BF16),
                pltpu.VMEM((CHUNKS, Q, D), BF16),
                pltpu.VMEM((KV_TOK // GRP, qw // hd, GRP, hd), F32),
                pltpu.VMEM((KV_TOK // GRP, qw // hd, GRP, hd), F32),
                pltpu.VMEM((KV_TOK // GRP, qw // hd * GRP, GRP * seq), BF16),
                pltpu.VMEM((M, qw + ff), BF16),
                pltpu.VMEM((tok, 128), jnp.int32),
                pltpu.VMEM((tok, 128), F32),
                dma((2, 2)), dma((3,)), dma((2, 3)), dma((2, 2)), dma((2 * CHUNKS,)),
                dma((3,)), dma((CHUNKS, 3, D // SUB)), dma((CHUNKS, 3)), dma((CHUNKS, 3)),
                dma((3,)), dma((3, D // SUB)), dma((2,)), dma((2,)), dma((2,)),
            ],
            compiler_params=pltpu.CompilerParams(
                collective_id=0, has_side_effects=True, vmem_limit_bytes=67043328),
            name="layers",
        )(x_in, len_in, freq, norm_gain, w_q, w_k, w_v, w_o, w_gate, w_up, w_down, kc, vc)[0]

    return jax.shard_map(per_device, mesh=mesh, in_specs=arg_specs, out_specs=P('dp', None), check_vma=False)
```
